32 devices in a mesh: data: 32 (over z, y, x, core).
Axes of the slice: x: 2, y: 2, z: 4, core: 2. Of those that a mesh axis runs over, the one named last changes fastest.
Arguments:
- x_in: bfloat16 [32768, 768], P('data')
- dy_in: bfloat16 [32768, 768], P('data')
- weights: bfloat16 [4, 768, 768], replicated
- a_old: float32 [3072, 768], P('data')
- s_old: float32 [3072, 768], P('data')
- a_inv: float32 [3072, 768], P('data')
- s_inv: float32 [4, 768, 768], replicated
Outputs:
- output 1: float32 [4, 768, 768], replicated
- output 2: float32 [3072, 768], P('data')
- output 3: float32 [3072, 768], P('data')
All inputs are finite; a program needn't handle non-finite values.
Results may differ from the reference program's by a relative error of at most 0.0010606.
Values are sent between devices in bfloat16 or wider.
A program may use at most 1 GiB of HBM per device.

```python
import functools
import jax
import jax.numpy as jnp

D = 768
LAYERS = 4
TOKENS = 1024
SHARDS = 32
LOW_RANK = 64
BATCH_TOTAL = TOKENS * SHARDS
FACTOR_DECAY = 0.75


def spd_stack(rng_key, base_diag, gram_scale):
    low_rank = jax.random.normal(rng_key, (LAYERS, D, LOW_RANK), jnp.float32)
    gram_mat = jnp.einsum("lir,ljr->lij", low_rank, low_rank)
    gram_mat = 0.5 * (gram_mat + jnp.swapaxes(gram_mat, 1, 2))
    return gram_scale * gram_mat + base_diag * jnp.eye(D, dtype=jnp.float32)


def shard_rows(rng_key, spread):
    key_raw, key_mean, key_scale = jax.random.split(rng_key, 3)
    raw_rows = jax.random.normal(key_raw, (SHARDS, TOKENS, D), jnp.float32)
    offset = 0.7 * jax.random.normal(key_mean, (SHARDS, 1, D), jnp.float32)
    row_scale = jnp.exp(spread * jax.random.normal(key_scale, (SHARDS, 1, 1), jnp.float32))
    return ((raw_rows + offset) * row_scale).reshape(BATCH_TOTAL, D).astype(jnp.bfloat16)


def setup_inputs(seed: int = 0) -> dict:
    key_list = jax.random.split(jax.random.key(seed), 7)
    weights = jax.random.normal(key_list[2], (LAYERS, D, D), jnp.float32) * D ** -0.5
    inv_scale = (LOW_RANK * D) ** -0.5
    return {
        "x_in": shard_rows(key_list[0], 0.5),
        "dy_in": shard_rows(key_list[1], 0.5),
        "weights": weights.astype(jnp.bfloat16),
        "a_old": spd_stack(key_list[3], 0.5, 1.0 / LOW_RANK).reshape(LAYERS * D, D),
        "s_old": spd_stack(key_list[4], 0.5, 1.0 / LOW_RANK).reshape(LAYERS * D, D),
        "a_inv": spd_stack(key_list[5], 0.5, inv_scale).reshape(LAYERS * D, D),
        "s_inv": spd_stack(key_list[6], 0.5, inv_scale),
    }


def gelu_grad(pre_act, d_act):
    pullback = jax.vjp(functools.partial(jax.nn.gelu, approximate=True), pre_act.astype(jnp.float32))[1]
    return pullback(d_act.astype(jnp.float32))[0].astype(jnp.bfloat16)


def reference(x_in, dy_in, weights, a_old, s_old, a_inv, s_inv):
    layer_inputs = [x_in]
    pre_acts = []
    for layer_id in range(LAYERS - 1):
        pre_act = jnp.dot(layer_inputs[layer_id], weights[layer_id], preferred_element_type=jnp.float32).astype(jnp.bfloat16)
        pre_acts.append(pre_act)
        layer_inputs.append(jax.nn.gelu(pre_act.astype(jnp.float32), approximate=True).astype(jnp.bfloat16))
    out_grads = [dy_in] * LAYERS
    for layer_id in range(LAYERS - 1, 0, -1):
        d_act = jnp.dot(out_grads[layer_id], weights[layer_id].T, preferred_element_type=jnp.float32).astype(jnp.bfloat16)
        out_grads[layer_id - 1] = gelu_grad(pre_acts[layer_id - 1], d_act)
    a_facs = []
    s_facs = []
    updates = []
    for layer_id in range(LAYERS):
        h_in = layer_inputs[layer_id]
        g_out = out_grads[layer_id]
        a_facs.append(jnp.dot(h_in.T, h_in, preferred_element_type=jnp.float32) / BATCH_TOTAL)
        s_facs.append(jnp.dot(g_out.T, g_out, preferred_element_type=jnp.float32) / BATCH_TOTAL)
        w_grad = jnp.dot(h_in.T, g_out, preferred_element_type=jnp.float32) / BATCH_TOTAL
        a_inv_layer = a_inv[layer_id * D:(layer_id + 1) * D]
        updates.append(jnp.dot(a_inv_layer, jnp.dot(w_grad, s_inv[layer_id])))
    a_new = FACTOR_DECAY * a_old + (1.0 - FACTOR_DECAY) * jnp.concatenate(a_facs, axis=0)
    s_new = FACTOR_DECAY * s_old + (1.0 - FACTOR_DECAY) * jnp.concatenate(s_facs, axis=0)
    return (jnp.stack(updates), a_new, s_new)
```

```python
import math
import jax
import jax.numpy as jnp
from jax import lax
from jax.experimental import pallas as pl
from jax.experimental.pallas import tpu as pltpu
from jax.sharding import PartitionSpec as P

DECAY = 0.75
F32 = jnp.float32
BF16 = jnp.bfloat16
MESH = pl.DeviceIdType.MESH
HIGH = lax.Precision.HIGHEST
LAYERS = 4
D = 768
ROWS = 1024
OWN = 96
HALF = 384
GELU_C = math.sqrt(2.0 / math.pi)
NT = (((1,), (1,)), ((), ()))

STEPS = 2560.0
BASE = 21.0
PAIR = OWN // 2
CODE = OWN + PAIR


def encode(v):
    hi = v.astype(BF16)
    h = hi.astype(F32)
    q = jnp.round((v - h) / jnp.where(h == 0.0, 1.0, h) * STEPS)
    q = jnp.clip(q, -10.0, 10.0)
    lo = q[:PAIR] * BASE + q[PAIR:]
    return hi, lo.astype(BF16)


def decode(hi, lo):
    h = hi.astype(F32)
    w = lo.astype(F32)
    top = jnp.round(w * (1.0 / BASE))
    q = jnp.concatenate([top, w - BASE * top], axis=-2)
    return h + h * (q * (1.0 / STEPS))


def put(ref, idx, v):
    hi, lo = encode(v)
    ref[(*idx, slice(0, OWN))] = hi
    ref[(*idx, slice(OWN, CODE))] = lo


def get(ref, idx):
    return decode(ref[(*idx, slice(0, OWN))], ref[(*idx, slice(OWN, CODE))])


def gelu_tanh(v):
    return jnp.tanh(GELU_C * (v + 0.044715 * (v * v * v)))


F, B, W, PR, T, C, Z, R, U, Y, V, AS = range(12)
EVENTS = [
    (F, 0), (W, 0), (PR, 4), (F, 1), (W, 7), (PR, 11), (F, 2), (W, 1), (PR, 5), (T, 4),
    (B, 3), (W, 3), (PR, 3), (B, 2), (W, 6), (W, 2), (PR, 2), (T, 11), (B, 1), (W, 5), (PR, 1), (T, 5), (C, 4),
    (W, 4), (PR, 0), (T, 3), (C, 11), (T, 2), (C, 5), (PR, 6), (C, 3), (T, 1), (C, 2), (T, 0), (PR, 7),
    (C, 1), (C, 0), (PR, 10), (Z, 0), (T, 6), (T, 7), (R, 0), (PR, 9), (PR, 8), (T, 10), (C, 6), (C, 7),
    (U, 0), (T, 9), (T, 8), (C, 10), (Y, 1), (V, 0), (Y, 2), (Y, 3), (C, 9), (C, 8), (V, 1), (V, 2), (V, 3), (AS, 0),
]


def kernel(
    x_hbm, dy_hbm, wt_hbm, w_hbm, sinv_hbm, a_old, s_old, a_inv,
    u_out, a_new, s_new,
    hg, wbuf, lhs, acc, accx, s1, r1, r2, zr, gcode, gfull, sinv, ubuf,
    lsem, wsem, d2d_s, d2d_r, s1_s, s1_r, s2_s, s2_r, z_s, z_r, g_s, g_r, uz_s, uz_r, u_s, u_r, us_loc,
):
    me = lax.axis_index("data")
    c = me % 2
    x = (me // 2) % 2
    y = (me // 4) % 2
    z = me // 8
    mate = me + 1 - 2 * c
    x_nbr = me + 2 - 4 * x
    y_nbr = me + 4 - 8 * y
    z_peer = [(me + 8 * k) % 32 for k in range(4)]

    def row_block(dy_, dx_):
        return 4 * ((y + dy_) % 2) + 2 * ((x + dx_) % 2) + c

    blocks = [row_block(0, 0), row_block(0, 1), row_block(1, 0), row_block(1, 1)]

    def rcopy(src, dst, ss, rs, dev):
        return pltpu.make_async_remote_copy(
            src_ref=src, dst_ref=dst, send_sem=ss, recv_sem=rs, device_id=(dev,), device_id_type=MESH
        )

    own = pl.ds(0, ROWS)
    far = pl.ds(ROWS, ROWS)
    ld_x = pltpu.make_async_copy(x_hbm, hg.at[0, :, own], lsem.at[0])
    ld_dy = pltpu.make_async_copy(dy_hbm, hg.at[7, :, own], lsem.at[1])
    ld_si = pltpu.make_async_copy(sinv_hbm.at[z], sinv, lsem.at[2])
    ld_x.start()
    ld_dy.start()
    for l in range(3):
        pltpu.make_async_copy(wt_hbm.at[l], wbuf.at[l], wsem.at[l]).start()
    ld_si.start()

    barrier = pltpu.get_barrier_semaphore()
    for dev in (mate, x_nbr, y_nbr, z_peer[1], z_peer[2], z_peer[3]):
        pl.semaphore_signal(barrier, inc=1, device_id=(dev,), device_id_type=MESH)
    pl.semaphore_wait(barrier, 6)

    def share(n):
        return rcopy(hg.at[n, :, own], hg.at[n, :, far], d2d_s.at[n], d2d_r.at[n], mate)

    def forward(l):
        pltpu.make_async_copy(wt_hbm.at[l], wbuf.at[l], wsem.at[l]).wait()

        @pl.loop(0, 3)
        def _(i):
            rows = pl.ds(pl.multiple_of(i * 256, 256), 256)
            pre = jnp.dot(wbuf[l, rows, :], hg[l, :, own], preferred_element_type=F32).astype(BF16)
            hg[4 + l, rows, own] = pre
            v = pre.astype(F32)
            hg[l + 1, rows, own] = (v * (0.5 * (1.0 + gelu_tanh(v)))).astype(BF16)

        share(l + 1).start()
        pltpu.make_async_copy(w_hbm.at[3 - l], wbuf.at[l], wsem.at[l]).start()

    def backward(l):
        k = 3 - l
        pltpu.make_async_copy(w_hbm.at[l], wbuf.at[k], wsem.at[k]).wait()

        @pl.loop(0, 3)
        def _(i):
            rows = pl.ds(pl.multiple_of(i * 256, 256), 256)
            dh = jnp.dot(wbuf[k, rows, :], hg[4 + l, :, own], preferred_element_type=F32).astype(BF16).astype(F32)
            v = hg[3 + l, rows, own].astype(F32)
            t = gelu_tanh(v)
            slope = 0.5 * (1.0 + t) + (0.5 * v) * (1.0 - t * t) * (GELU_C * (1.0 + (3.0 * 0.044715) * (v * v)))
            hg[3 + l, rows, own] = (dh * slope).astype(BF16)

        share(3 + l).start()

    def st1(m, j):
        return rcopy(s1.at[m, j], r1.at[m, j], s1_s.at[m, j], s1_r.at[m, j], (x_nbr, y_nbr)[j])

    def st2(m, j):
        return rcopy(s1.at[m, 0, j], r2.at[m, j], s2_s.at[m, j], s2_r.at[m, j], (y_nbr, x_nbr)[j])

    def product(m):
        kind = m // 4
        l = m % 4
        left = jnp.where(kind == 2, 4 + l, l)
        right = jnp.where(kind == 1, l, 4 + l)
        for d in range(4):
            lhs[pl.ds(OWN * d, OWN), :] = hg[left, pl.ds(pl.multiple_of(blocks[d] * OWN, OWN), OWN), :]

        @pl.loop(0, 2)
        def _(j):
            cols = pl.ds(pl.multiple_of(j * HALF, HALF), HALF)
            out = lax.dot_general(lhs[...], hg[right, cols, :], NT, preferred_element_type=F32)
            acc[m, :, cols] = out[0:OWN]
            first = out[OWN : 2 * OWN]
            second = out[2 * OWN : 3 * OWN]
            put(s1, (m, j, 0), jnp.where(j == 0, first, second))
            accx[m, j] = jnp.where(j == 0, second, first)
            put(s1, (m, j, 1), out[3 * OWN :])

        for j in range(2):
            st1(m, j).start()

    def turn(m):
        st1(m, 0).wait_send()
        for j in range(2):
            st1(m, j).wait_recv()
            put(s1, (m, 0, j), accx[m, j] + get(r1, (m, j, 1)))
            st2(m, j).start()
            acc[m, :, pl.ds(j * HALF, HALF)] += get(r1, (m, j, 0))

    def z_copy(m):
        kind = m // 4
        l = m % 4
        slot = (l - z + 3) % 4
        return rcopy(s1.at[m, 1], zr.at[kind, slot], z_s.at[m], z_r.at[kind, slot], (me + 8 * (l - z) + 32) % 32)

    def across(m):
        st1(m, 1).wait_send()
        for j in range(2):
            st2(m, j).wait_recv()
            total = acc[m, :, pl.ds(j * HALF, HALF)] + get(r2, (m, j))
            acc[m, :, pl.ds(j * HALF, HALF)] = total

            @pl.when(m % 4 != z)
            def _():
                put(s1, (m, 1, j), total)

        @pl.when(m % 4 != z)
        def _():
            z_copy(m).start()

    def z_total(kind, j):
        t = acc[kind * 4 + z, :, pl.ds(j * HALF, HALF)]
        for k in range(3):
            t = t + get(zr, (kind, k, j))
        return t

    def z_wait(kind):
        for k in range(3):
            rcopy(s1.at[0, 1], zr.at[kind, k], z_s.at[0], z_r.at[kind, k], z_peer[k + 1]).wait_recv()

    inv_batch = 1.0 / (ROWS * 32)

    def gather_copies(ref, base, ss, rs, own_src):
        def at(rb, half=None):
            return ref.at[base + rb] if half is None else ref.at[base + rb, half]

        first = [
            rcopy(own_src, at(blocks[0]), ss.at[0], rs.at[0], x_nbr),
            rcopy(own_src, at(blocks[0]), ss.at[1], rs.at[1], y_nbr),
            rcopy(own_src, at(blocks[0]), ss.at[2], rs.at[2], mate),
        ]
        from_x = [
            rcopy(at(blocks[1], 0), at(blocks[1], 0), ss.at[3], rs.at[3], y_nbr),
            rcopy(at(blocks[1]), at(blocks[1]), ss.at[5], rs.at[5], mate),
        ]
        from_y = [
            rcopy(at(blocks[2], 1), at(blocks[2], 1), ss.at[4], rs.at[4], x_nbr),
            rcopy(at(blocks[2]), at(blocks[2]), ss.at[6], rs.at[6], mate),
        ]
        last = rcopy(at(blocks[3]), at(blocks[3]), ss.at[7], rs.at[7], mate)
        return first, from_x, from_y, last

    def gather_rest(copies):
        first, from_x, from_y, last = copies
        first[0].wait_recv()
        for cp in from_x:
            cp.start()
        first[1].wait_recv()
        for cp in from_y:
            cp.start()
        from_x[0].wait_recv()
        from_y[0].wait_recv()
        last.start()

    def gather_end(copies):
        first, from_x, from_y, last = copies
        for cp in (first[2], from_x[1], from_y[1], last):
            cp.wait_recv()

    def gather_sent(copies):
        first, from_x, from_y, last = copies
        for cp in (*first, *from_x, *from_y, last):
            cp.wait_send()

    g_copies = gather_copies(gcode, 0, g_s, g_r, gcode.at[blocks[0]])

    def u_row(l):
        return u_out.at[l * 8 + blocks[0]]

    def u_copies(k):
        l = (z - k + 4) % 4
        return gather_copies(u_out, l * 8, u_s.at[k], u_r.at[k], u_row(l))

    own_first = gather_copies(u_out, z * 8, u_s.at[0], u_r.at[0], ubuf)[0]
    local = pltpu.make_async_copy(ubuf, u_row(z), us_loc)

    def z_send(k, l):
        return rcopy(ubuf, u_row(l), uz_s.at[k - 1], uz_r.at[k - 1], (me + 8 * k) % 32)

    def own_grad(_):
        z_wait(0)
        for j in range(2):
            put(gcode, (blocks[0], j), z_total(0, j) * inv_batch)
        for cp in g_copies[0]:
            cp.start()

    def precondition(_):
        gather_end(g_copies)

        @pl.loop(0, 8)
        def _(b):
            for j in range(2):
                gfull[pl.ds(pl.multiple_of(b * OWN, OWN), OWN), pl.ds(j * HALF, HALF)] = get(gcode, (b, j))

        ld_si.wait()
        left_prod = jnp.dot(a_inv[...], gfull[...], precision=HIGH, preferred_element_type=F32)
        u_rows = jnp.dot(left_prod, sinv[...], precision=HIGH, preferred_element_type=F32)
        for j in range(2):
            put(ubuf, (j,), u_rows[:, j * HALF : (j + 1) * HALF])
        for k in range(1, 4):
            z_send(k, z).start()
        for cp in own_first:
            cp.start()
        local.start()

    def from_plane(k):
        z_send(k, (z - k + 4) % 4).wait_recv()
        for cp in u_copies(k)[0]:
            cp.start()

    def factors(_):
        for kind, old, new in ((1, a_old, a_new), (2, s_old, s_new)):
            z_wait(kind)
            for j in range(2):
                cols = pl.ds(j * HALF, HALF)
                new[:, cols] = DECAY * old[:, cols] + ((1.0 - DECAY) * inv_batch) * z_total(kind, j)

    ld_x.wait()
    share(0).start()
    ld_dy.wait()
    share(7).start()

    actions = {
        F: forward,
        B: backward,
        W: lambda n: share(n).wait_recv(),
        PR: product,
        T: turn,
        C: across,
        Z: own_grad,
        R: lambda _: gather_rest(g_copies),
        U: precondition,
        Y: from_plane,
        V: lambda k: gather_rest(u_copies(k)),
        AS: factors,
    }

    @pl.loop(0, len(EVENTS))
    def _(step):
        code = jnp.int32(0)
        for s, (op, arg) in enumerate(EVENTS):
            code = jnp.where(step == s, op * 16 + arg, code)
        op = code // 16
        arg = code % 16
        for o, act in actions.items():

            @pl.when(op == o)
            def _(act=act):
                act(arg)

    @pl.loop(0, 4)
    def _(k):
        gather_end(u_copies(k))
        gather_sent(u_copies(k))

    for k in range(1, 4):
        z_send(k, z).wait_send()
    local.wait()
    gather_sent(g_copies)

    @pl.loop(0, 8)
    def _(n):
        share(n).wait_send()

    @pl.loop(0, 12)
    def _(m):
        for j in range(2):
            st2(m, j).wait_send()

        @pl.when(m % 4 != z)
        def _():
            z_copy(m).wait_send()


def open_rows(code, rows):
    for b in range(4):
        for j in range(2):
            rows[0, b * OWN : (b + 1) * OWN, j * HALF : (j + 1) * HALF] = get(code, (b, j))


def solution(mesh):
    def device_step(x_loc, dy_loc, weights, a_old_rows, s_old_rows, a_inv_rows, s_inv):
        any_spec = pl.BlockSpec(memory_space=pl.ANY)
        vmem = pl.BlockSpec(memory_space=pltpu.VMEM)
        dma = pltpu.SemaphoreType.DMA
        u_code, a_new, s_new = pl.pallas_call(
            kernel,
            out_shape=(
                jax.ShapeDtypeStruct((LAYERS * 8, 2, CODE, HALF), BF16),
                jax.ShapeDtypeStruct((OWN, D), F32),
                jax.ShapeDtypeStruct((OWN, D), F32),
            ),
            in_specs=[any_spec] * 5 + [vmem] * 3,
            out_specs=(any_spec, vmem, vmem),
            scratch_shapes=[
                pltpu.VMEM((2 * LAYERS, D, 2 * ROWS), BF16),
                pltpu.VMEM((3, D, D), BF16),
                pltpu.VMEM((4 * OWN, 2 * ROWS), BF16),
                pltpu.VMEM((12, OWN, D), F32),
                pltpu.VMEM((12, 2, OWN, HALF), F32),
                pltpu.VMEM((12, 2, 2, CODE, HALF), BF16),
                pltpu.VMEM((12, 2, 2, CODE, HALF), BF16),
                pltpu.VMEM((12, 2, CODE, HALF), BF16),
                pltpu.VMEM((3, 3, 2, CODE, HALF), BF16),
                pltpu.VMEM((8, 2, CODE, HALF), BF16),
                pltpu.VMEM((D, D), F32),
                pltpu.VMEM((D, D), F32),
                pltpu.VMEM((2, CODE, HALF), BF16),
                dma((3,)),
                dma((3,)),
                dma((8,)), dma((8,)),
                dma((12, 2)), dma((12, 2)),
                dma((12, 2)), dma((12, 2)),
                dma((12,)), dma((3, 3)),
                dma((8,)), dma((8,)),
                dma((3,)), dma((3,)),
                dma((4, 8)), dma((4, 8)),
                dma,
            ],
            compiler_params=pltpu.CompilerParams(
                collective_id=0, has_side_effects=True, vmem_limit_bytes=67_000_000
            ),
        )(x_loc.T, dy_loc.T, jnp.swapaxes(weights[:3], 1, 2), weights, s_inv, a_old_rows, s_old_rows, a_inv_rows)
        u_pre = pl.pallas_call(
            open_rows,
            out_shape=jax.ShapeDtypeStruct((LAYERS, D, D), F32),
            grid=(8,),
            in_specs=[pl.BlockSpec((4, 2, CODE, HALF), lambda i: (i, 0, 0, 0))],
            out_specs=pl.BlockSpec((1, 4 * OWN, D), lambda i: (i // 2, i % 2, 0)),
        )(u_code)
        return u_pre, a_new, s_new

    row_spec = P("data", None)
    return jax.shard_map(
        device_step,
        mesh=mesh,
        in_specs=(row_spec, row_spec, P(), row_spec, row_spec, row_spec, P()),
        out_specs=(P(), row_spec, row_spec),
        check_vma=False,
    )
```

```python
import math
import jax
import jax.numpy as jnp
from jax import lax
from jax.experimental import pallas as pl
from jax.experimental.pallas import tpu as pltpu
from jax.sharding import PartitionSpec as P

DECAY = 0.75
F32 = jnp.float32
BF16 = jnp.bfloat16
MESH = pl.DeviceIdType.MESH
HIGH = lax.Precision.HIGHEST
LAYERS = 4
D = 768
ROWS = 1024
OWN = 96
HALF = 384
GELU_C = math.sqrt(2.0 / math.pi)
NT = (((1,), (1,)), ((), ()))

STEPS = 2560.0
BASE = 21.0
PAIR = OWN // 2
CODE = OWN + PAIR


def encode(v):
    hi = v.astype(BF16)
    h = hi.astype(F32)
    q = jnp.round((v - h) / jnp.where(h == 0.0, 1.0, h) * STEPS)
    q = jnp.clip(q, -10.0, 10.0)
    lo = q[:PAIR] * BASE + q[PAIR:]
    return hi, lo.astype(BF16)


def decode(hi, lo):
    h = hi.astype(F32)
    w = lo.astype(F32)
    top = jnp.round(w * (1.0 / BASE))
    q = jnp.concatenate([top, w - BASE * top], axis=-2)
    return h + h * (q * (1.0 / STEPS))


def put(ref, idx, v):
    hi, lo = encode(v)
    ref[(*idx, slice(0, OWN))] = hi
    ref[(*idx, slice(OWN, CODE))] = lo


def get(ref, idx):
    return decode(ref[(*idx, slice(0, OWN))], ref[(*idx, slice(OWN, CODE))])


def gelu_tanh(v):
    return jnp.tanh(GELU_C * (v + 0.044715 * (v * v * v)))


F, B, W, PR, T, C, Z, R, U, Y, V, AS, RQ, VQ = range(14)
EVENTS = [
    (F, 0), (W, 0), (PR, 4), (W, 7), (PR, 11), (W, 1), (PR, 5), (F, 1), (F, 2), (T, 4),
    (B, 3), (B, 2), (T, 5), (W, 5), (PR, 1), (W, 3), (PR, 3), (C, 5), (W, 2), (W, 6),
    (PR, 2), (T, 1), (B, 1), (T, 3), (W, 4), (PR, 0), (T, 2), (C, 3), (T, 0), (C, 1),
    (PR, 6), (C, 2), (T, 11), (PR, 9), (C, 0), (T, 6), (T, 9), (C, 6), (Z, 0), (C, 11),
    (C, 4), (R, 0), (PR, 8), (PR, 10), (RQ, 0), (U, 0), (T, 10), (PR, 7), (T, 8), (T, 7),
    (C, 10), (Y, 1), (C, 7), (C, 8), (C, 9), (Y, 2), (V, 1), (Y, 3), (V, 2), (V, 0),
    (V, 3), (VQ, 0), (VQ, 2), (VQ, 1), (VQ, 3), (AS, 0),
]


def kernel(
    x_hbm, dy_hbm, wt_hbm, w_hbm, sinv_hbm, a_old, s_old, a_inv,
    u_out, a_new, s_new,
    hg, wbuf, lhs, acc, accx, s1, r1, r2, zr, gcode, gfull, sinv, ubuf,
    lsem, wsem, d2d_s, d2d_r, s1_s, s1_r, s2_s, s2_r, z_s, z_r, g_s, g_r, uz_s, uz_r, u_s, u_r, us_loc,
):
    me = lax.axis_index("data")
    c = me % 2
    x = (me // 2) % 2
    y = (me // 4) % 2
    z = me // 8
    mate = me + 1 - 2 * c
    x_nbr = me + 2 - 4 * x
    y_nbr = me + 4 - 8 * y
    z_peer = [(me + 8 * k) % 32 for k in range(4)]

    def row_block(dy_, dx_):
        return 4 * ((y + dy_) % 2) + 2 * ((x + dx_) % 2) + c

    blocks = [row_block(0, 0), row_block(0, 1), row_block(1, 0), row_block(1, 1)]

    def rcopy(src, dst, ss, rs, dev):
        return pltpu.make_async_remote_copy(
            src_ref=src, dst_ref=dst, send_sem=ss, recv_sem=rs, device_id=(dev,), device_id_type=MESH
        )

    own = pl.ds(0, ROWS)
    far = pl.ds(ROWS, ROWS)
    ld_x = pltpu.make_async_copy(x_hbm, hg.at[0, :, own], lsem.at[0])
    ld_dy = pltpu.make_async_copy(dy_hbm, hg.at[7, :, own], lsem.at[1])
    ld_si = pltpu.make_async_copy(sinv_hbm.at[z], sinv, lsem.at[2])
    ld_x.start()
    ld_dy.start()
    for l in range(3):
        pltpu.make_async_copy(wt_hbm.at[l], wbuf.at[l], wsem.at[l]).start()
    ld_si.start()

    barrier = pltpu.get_barrier_semaphore()
    for dev in (mate, x_nbr, y_nbr, z_peer[1], z_peer[2], z_peer[3]):
        pl.semaphore_signal(barrier, inc=1, device_id=(dev,), device_id_type=MESH)
    pl.semaphore_wait(barrier, 6)

    def share(n):
        return rcopy(hg.at[n, :, own], hg.at[n, :, far], d2d_s.at[n], d2d_r.at[n], mate)

    def forward(l):
        pltpu.make_async_copy(wt_hbm.at[l], wbuf.at[l], wsem.at[l]).wait()

        @pl.loop(0, 3)
        def _(i):
            rows = pl.ds(pl.multiple_of(i * 256, 256), 256)
            pre = jnp.dot(wbuf[l, rows, :], hg[l, :, own], preferred_element_type=F32).astype(BF16)
            hg[4 + l, rows, own] = pre
            v = pre.astype(F32)
            hg[l + 1, rows, own] = (v * (0.5 * (1.0 + gelu_tanh(v)))).astype(BF16)

        share(l + 1).start()
        pltpu.make_async_copy(w_hbm.at[3 - l], wbuf.at[l], wsem.at[l]).start()

    def backward(l):
        k = 3 - l
        pltpu.make_async_copy(w_hbm.at[l], wbuf.at[k], wsem.at[k]).wait()

        @pl.loop(0, 3)
        def _(i):
            rows = pl.ds(pl.multiple_of(i * 256, 256), 256)
            dh = jnp.dot(wbuf[k, rows, :], hg[4 + l, :, own], preferred_element_type=F32).astype(BF16).astype(F32)
            v = hg[3 + l, rows, own].astype(F32)
            t = gelu_tanh(v)
            slope = 0.5 * (1.0 + t) + (0.5 * v) * (1.0 - t * t) * (GELU_C * (1.0 + (3.0 * 0.044715) * (v * v)))
            hg[3 + l, rows, own] = (dh * slope).astype(BF16)

        share(3 + l).start()

    def st1(m, j):
        return rcopy(s1.at[m, j], r1.at[m, j], s1_s.at[m, j], s1_r.at[m, j], (x_nbr, y_nbr)[j])

    def st2(m, j):
        return rcopy(s1.at[m, 0, j], r2.at[m, j], s2_s.at[m, j], s2_r.at[m, j], (y_nbr, x_nbr)[j])

    def product(m):
        kind = m // 4
        l = m % 4
        left = jnp.where(kind == 2, 4 + l, l)
        right = jnp.where(kind == 1, l, 4 + l)
        for d in range(4):
            lhs[pl.ds(OWN * d, OWN), :] = hg[left, pl.ds(pl.multiple_of(blocks[d] * OWN, OWN), OWN), :]

        @pl.loop(0, 2)
        def _(j):
            cols = pl.ds(pl.multiple_of(j * HALF, HALF), HALF)
            out = lax.dot_general(lhs[...], hg[right, cols, :], NT, preferred_element_type=F32)
            acc[m, :, cols] = out[0:OWN]
            first = out[OWN : 2 * OWN]
            second = out[2 * OWN : 3 * OWN]
            put(s1, (m, j, 0), jnp.where(j == 0, first, second))
            accx[m, j] = jnp.where(j == 0, second, first)
            put(s1, (m, j, 1), out[3 * OWN :])

        for j in range(2):
            st1(m, j).start()

    def turn(m):
        st1(m, 0).wait_send()
        for j in range(2):
            st1(m, j).wait_recv()
            put(s1, (m, 0, j), accx[m, j] + get(r1, (m, j, 1)))
            st2(m, j).start()
            acc[m, :, pl.ds(j * HALF, HALF)] += get(r1, (m, j, 0))

    def z_copy(m):
        kind = m // 4
        l = m % 4
        slot = (l - z + 3) % 4
        return rcopy(s1.at[m, 1], zr.at[kind, slot], z_s.at[m], z_r.at[kind, slot], (me + 8 * (l - z) + 32) % 32)

    def across(m):
        st1(m, 1).wait_send()
        for j in range(2):
            st2(m, j).wait_recv()
            total = acc[m, :, pl.ds(j * HALF, HALF)] + get(r2, (m, j))
            acc[m, :, pl.ds(j * HALF, HALF)] = total

            @pl.when(m % 4 != z)
            def _():
                put(s1, (m, 1, j), total)

        @pl.when(m % 4 != z)
        def _():
            z_copy(m).start()

    def z_total(kind, j):
        t = acc[kind * 4 + z, :, pl.ds(j * HALF, HALF)]
        for k in range(3):
            t = t + get(zr, (kind, k, j))
        return t

    def z_wait(kind):
        for k in range(3):
            rcopy(s1.at[0, 1], zr.at[kind, k], z_s.at[0], z_r.at[kind, k], z_peer[k + 1]).wait_recv()

    inv_batch = 1.0 / (ROWS * 32)

    def gather_copies(ref, base, ss, rs, own_src):
        def at(rb, half=None):
            return ref.at[base + rb] if half is None else ref.at[base + rb, half]

        first = [
            rcopy(own_src, at(blocks[0]), ss.at[0], rs.at[0], x_nbr),
            rcopy(own_src, at(blocks[0]), ss.at[1], rs.at[1], y_nbr),
            rcopy(own_src, at(blocks[0]), ss.at[2], rs.at[2], mate),
        ]
        from_x = [
            rcopy(at(blocks[1], 0), at(blocks[1], 0), ss.at[3], rs.at[3], y_nbr),
            rcopy(at(blocks[1]), at(blocks[1]), ss.at[5], rs.at[5], mate),
        ]
        from_y = [
            rcopy(at(blocks[2], 1), at(blocks[2], 1), ss.at[4], rs.at[4], x_nbr),
            rcopy(at(blocks[2]), at(blocks[2]), ss.at[6], rs.at[6], mate),
        ]
        last = rcopy(at(blocks[3]), at(blocks[3]), ss.at[7], rs.at[7], mate)
        return first, from_x, from_y, last

    def gather_rest(copies):
        first, from_x, from_y, last = copies
        first[0].wait_recv()
        for cp in from_x:
            cp.start()
        first[1].wait_recv()
        for cp in from_y:
            cp.start()

    def gather_last(copies):
        first, from_x, from_y, last = copies
        from_x[0].wait_recv()
        from_y[0].wait_recv()
        last.start()

    def gather_end(copies):
        first, from_x, from_y, last = copies
        for cp in (first[2], from_x[1], from_y[1], last):
            cp.wait_recv()

    def gather_sent(copies):
        first, from_x, from_y, last = copies
        for cp in (*first, *from_x, *from_y, last):
            cp.wait_send()

    g_copies = gather_copies(gcode, 0, g_s, g_r, gcode.at[blocks[0]])

    def u_row(l):
        return u_out.at[l * 8 + blocks[0]]

    def u_copies(k):
        l = (z - k + 4) % 4
        return gather_copies(u_out, l * 8, u_s.at[k], u_r.at[k], u_row(l))

    own_first = gather_copies(u_out, z * 8, u_s.at[0], u_r.at[0], ubuf)[0]
    local = pltpu.make_async_copy(ubuf, u_row(z), us_loc)

    def z_send(k, l):
        return rcopy(ubuf, u_row(l), uz_s.at[k - 1], uz_r.at[k - 1], (me + 8 * k) % 32)

    def own_grad(_):
        z_wait(0)
        for j in range(2):
            put(gcode, (blocks[0], j), z_total(0, j) * inv_batch)
        for cp in g_copies[0]:
            cp.start()

    def precondition(_):
        gather_end(g_copies)

        @pl.loop(0, 8)
        def _(b):
            for j in range(2):
                gfull[pl.ds(pl.multiple_of(b * OWN, OWN), OWN), pl.ds(j * HALF, HALF)] = get(gcode, (b, j))

        ld_si.wait()
        left_prod = jnp.dot(a_inv[...], gfull[...], precision=HIGH, preferred_element_type=F32)
        u_rows = jnp.dot(left_prod, sinv[...], precision=HIGH, preferred_element_type=F32)
        for j in range(2):
            put(ubuf, (j,), u_rows[:, j * HALF : (j + 1) * HALF])
        for k in range(1, 4):
            z_send(k, z).start()
        for cp in own_first:
            cp.start()
        local.start()

    def from_plane(k):
        z_send(k, (z - k + 4) % 4).wait_recv()
        for cp in u_copies(k)[0]:
            cp.start()

    def factors(_):
        for kind, old, new in ((1, a_old, a_new), (2, s_old, s_new)):
            z_wait(kind)
            for j in range(2):
                cols = pl.ds(j * HALF, HALF)
                new[:, cols] = DECAY * old[:, cols] + ((1.0 - DECAY) * inv_batch) * z_total(kind, j)

    ld_x.wait()
    share(0).start()
    ld_dy.wait()
    share(7).start()

    actions = {
        F: forward,
        B: backward,
        W: lambda n: share(n).wait_recv(),
        PR: product,
        T: turn,
        C: across,
        Z: own_grad,
        R: lambda _: gather_rest(g_copies),
        U: precondition,
        Y: from_plane,
        V: lambda k: gather_rest(u_copies(k)),
        AS: factors,
        RQ: lambda _: gather_last(g_copies),
        VQ: lambda k: gather_last(u_copies(k)),
    }

    @pl.loop(0, len(EVENTS))
    def _(step):
        code = jnp.int32(0)
        for s, (op, arg) in enumerate(EVENTS):
            code = jnp.where(step == s, op * 16 + arg, code)
        op = code // 16
        arg = code % 16
        for o, act in actions.items():

            @pl.when(op == o)
            def _(act=act):
                act(arg)

    @pl.loop(0, 4)
    def _(k):
        gather_end(u_copies(k))
        gather_sent(u_copies(k))

    for k in range(1, 4):
        z_send(k, z).wait_send()
    local.wait()
    gather_sent(g_copies)

    @pl.loop(0, 8)
    def _(n):
        share(n).wait_send()

    @pl.loop(0, 12)
    def _(m):
        for j in range(2):
            st2(m, j).wait_send()

        @pl.when(m % 4 != z)
        def _():
            z_copy(m).wait_send()


def open_rows(code, rows):
    for b in range(4):
        for j in range(2):
            rows[0, b * OWN : (b + 1) * OWN, j * HALF : (j + 1) * HALF] = get(code, (b, j))


def solution(mesh):
    def device_step(x_loc, dy_loc, weights, a_old_rows, s_old_rows, a_inv_rows, s_inv):
        any_spec = pl.BlockSpec(memory_space=pl.ANY)
        vmem = pl.BlockSpec(memory_space=pltpu.VMEM)
        dma = pltpu.SemaphoreType.DMA
        u_code, a_new, s_new = pl.pallas_call(
            kernel,
            out_shape=(
                jax.ShapeDtypeStruct((LAYERS * 8, 2, CODE, HALF), BF16),
                jax.ShapeDtypeStruct((OWN, D), F32),
                jax.ShapeDtypeStruct((OWN, D), F32),
            ),
            in_specs=[any_spec] * 5 + [vmem] * 3,
            out_specs=(any_spec, vmem, vmem),
            scratch_shapes=[
                pltpu.VMEM((2 * LAYERS, D, 2 * ROWS), BF16),
                pltpu.VMEM((3, D, D), BF16),
                pltpu.VMEM((4 * OWN, 2 * ROWS), BF16),
                pltpu.VMEM((12, OWN, D), F32),
                pltpu.VMEM((12, 2, OWN, HALF), F32),
                pltpu.VMEM((12, 2, 2, CODE, HALF), BF16),
                pltpu.VMEM((12, 2, 2, CODE, HALF), BF16),
                pltpu.VMEM((12, 2, CODE, HALF), BF16),
                pltpu.VMEM((3, 3, 2, CODE, HALF), BF16),
                pltpu.VMEM((8, 2, CODE, HALF), BF16),
                pltpu.VMEM((D, D), F32),
                pltpu.VMEM((D, D), F32),
                pltpu.VMEM((2, CODE, HALF), BF16),
                dma((3,)),
                dma((3,)),
                dma((8,)), dma((8,)),
                dma((12, 2)), dma((12, 2)),
                dma((12, 2)), dma((12, 2)),
                dma((12,)), dma((3, 3)),
                dma((8,)), dma((8,)),
                dma((3,)), dma((3,)),
                dma((4, 8)), dma((4, 8)),
                dma,
            ],
            compiler_params=pltpu.CompilerParams(
                collective_id=0, has_side_effects=True, vmem_limit_bytes=67_000_000
            ),
        )(x_loc.T, dy_loc.T, jnp.swapaxes(weights[:3], 1, 2), weights, s_inv, a_old_rows, s_old_rows, a_inv_rows)
        u_pre = pl.pallas_call(
            open_rows,
            out_shape=jax.ShapeDtypeStruct((LAYERS, D, D), F32),
            grid=(8,),
            in_specs=[pl.BlockSpec((4, 2, CODE, HALF), lambda i: (i, 0, 0, 0))],
            out_specs=pl.BlockSpec((1, 4 * OWN, D), lambda i: (i // 2, i % 2, 0)),
        )(u_code)
        return u_pre, a_new, s_new

    row_spec = P("data", None)
    return jax.shard_map(
        device_step,
        mesh=mesh,
        in_specs=(row_spec, row_spec, P(), row_spec, row_spec, row_spec, P()),
        out_specs=(P(), row_spec, row_spec),
        check_vma=False,
    )
```

```python
import math
import jax
import jax.numpy as jnp
from jax import lax
from jax.experimental import pallas as pl
from jax.experimental.pallas import tpu as pltpu
from jax.sharding import PartitionSpec as P

DECAY = 0.75
F32 = jnp.float32
BF16 = jnp.bfloat16
MESH = pl.DeviceIdType.MESH
HIGH = lax.Precision.HIGHEST
LAYERS = 4
D = 768
ROWS = 1024
BATCH = 32 * ROWS
OWN = 96
HALF = 384
BAND = 512
BHALF = BAND // 2
GELU_C = math.sqrt(2.0 / math.pi)
NT = (((1,), (1,)), ((), ()))
TN = (((0,), (0,)), ((), ()))

STEPS = 2560.0
BASE = 21.0
PAIR = OWN // 2
CODE = OWN + PAIR


def nearest(v):
    return (v + 12582912.0) - 12582912.0


def encode(v):
    hi = v.astype(BF16)
    h = hi.astype(F32)
    q = nearest(jnp.clip((v - h) / jnp.where(h == 0.0, 1.0, h) * STEPS, -10.0, 10.0))
    lo = q[:PAIR] * BASE + q[PAIR:]
    return hi, lo.astype(BF16)


def decode(hi, lo):
    h = hi.astype(F32)
    w = lo.astype(F32)
    top = nearest(w * (1.0 / BASE))
    q = jnp.concatenate([top, w - BASE * top], axis=-2)
    return h + h * (q * (1.0 / STEPS))


def put(ref, idx, v):
    hi, lo = encode(v)
    ref[(*idx, slice(0, OWN))] = hi
    ref[(*idx, slice(OWN, CODE))] = lo


def get(ref, idx):
    return decode(ref[(*idx, slice(0, OWN))], ref[(*idx, slice(OWN, CODE))])


def gelu_tanh(v):
    return jnp.tanh(GELU_C * (v + 0.044715 * (v * v * v)))


F, B, W, PR, T, C, Z, R, U, Y, V, AS, RQ, VQ, DY = range(15)
EVENTS = [
    (F, 0), (DY, 0), (W, 0), (PR, 4), (W, 7), (PR, 11), (W, 1), (PR, 5), (F, 1), (F, 2), (T, 4),
    (B, 3), (B, 2), (T, 5), (W, 5), (PR, 1), (W, 3), (PR, 3), (C, 5), (W, 2), (W, 6),
    (PR, 2), (T, 1), (B, 1), (T, 3), (W, 4), (PR, 0), (T, 2), (C, 3), (T, 0), (C, 1),
    (PR, 6), (C, 2), (T, 11), (PR, 9), (C, 0), (T, 6), (T, 9), (C, 6), (Z, 0), (C, 11),
    (C, 4), (R, 0), (PR, 8), (PR, 10), (RQ, 0), (U, 0), (T, 10), (PR, 7), (T, 8), (T, 7),
    (C, 10), (Y, 1), (C, 7), (C, 8), (C, 9), (Y, 2), (V, 1), (Y, 3), (V, 2), (V, 0),
    (V, 3), (VQ, 0), (VQ, 2), (VQ, 1), (VQ, 3), (AS, 0),
]


def kernel(
    x_hbm, dy_hbm, w_hbm, sinv_hbm, a_inv,
    u_out, f_sum, f_flip,
    hg, wbuf, lhs, full, accg, accxg, s1g, r1g, r2g, zrg, accs, accxs, s1s, r1s, r2s, zrs, flip, gcode, gfull, sinv, ubuf,
    in_sem, lsem, wsem, d2d_s, d2d_r, s1_s, s1_r, s2_s, s2_r, z_s, z_r, t_s, t_r, g_s, g_r, uz_s, uz_r, u_s, u_r, us_loc,
):
    me = lax.axis_index("data")
    c = me % 2
    x = (me // 2) % 2
    y = (me // 4) % 2
    z = me // 8
    mate = me + 1 - 2 * c
    x_nbr = me + 2 - 4 * x
    y_nbr = me + 4 - 8 * y
    z_peer = [(me + 8 * k) % 32 for k in range(4)]

    def row_block(dy_, dx_):
        return 4 * ((y + dy_) % 2) + 2 * ((x + dx_) % 2) + c

    blocks = [row_block(0, 0), row_block(0, 1), row_block(1, 0), row_block(1, 1)]

    def rcopy(src, dst, ss, rs, dev):
        return pltpu.make_async_remote_copy(
            src_ref=src, dst_ref=dst, send_sem=ss, recv_sem=rs, device_id=(dev,), device_id_type=MESH
        )

    own = pl.ds(0, ROWS)
    far = pl.ds(ROWS, ROWS)
    def stage(i, j, k):
        return (s1g.at[i, j, k] if i < 4 else gcode.at[2 * (i - 4) + k, j]).at[pl.ds(0, 128)]

    def piece(k, i, j):
        src = (x_hbm, dy_hbm)[k].at[pl.ds(128 * i, 128), pl.ds(HALF * j, HALF)]
        return pltpu.make_async_copy(src, stage(i, j, k), in_sem.at[k, i, j])

    ld_si = pltpu.make_async_copy(sinv_hbm.at[z], sinv, lsem)
    for k in range(2):
        for i in range(8):
            for j in range(2):
                piece(k, i, j).start()
    for l in range(3):
        pltpu.make_async_copy(w_hbm.at[l], wbuf.at[l], wsem.at[l]).start()
    ld_si.start()

    barrier = pltpu.get_barrier_semaphore()
    for dev in [z * 8 + (me + k) % 8 for k in range(1, 8)] + z_peer[1:]:
        pl.semaphore_signal(barrier, inc=1, device_id=(dev,), device_id_type=MESH)
    pl.semaphore_wait(barrier, 10)

    def share(n):
        return rcopy(hg.at[n, :, own], hg.at[n, :, far], d2d_s.at[n], d2d_r.at[n], mate)

    def forward(l):
        pltpu.make_async_copy(w_hbm.at[l], wbuf.at[l], wsem.at[l]).wait()

        @pl.loop(0, 3)
        def _(i):
            rows = pl.ds(pl.multiple_of(i * 256, 256), 256)
            pre = lax.dot_general(wbuf[l, :, rows], hg[l, :, own], TN, preferred_element_type=F32).astype(BF16)
            hg[4 + l, rows, own] = pre
            v = pre.astype(F32)
            hg[l + 1, rows, own] = (v * (0.5 * (1.0 + gelu_tanh(v)))).astype(BF16)

        share(l + 1).start()

        @pl.when(l == 0)
        def _():
            pltpu.make_async_copy(w_hbm.at[3], wbuf.at[0], wsem.at[0]).start()

    def backward(l):
        k = l % 3

        @pl.when(l == 3)
        def _():
            pltpu.make_async_copy(w_hbm.at[3], wbuf.at[0], wsem.at[0]).wait()

        @pl.loop(0, 3)
        def _(i):
            rows = pl.ds(pl.multiple_of(i * 256, 256), 256)
            dh = jnp.dot(wbuf[k, rows, :], hg[4 + l, :, own], preferred_element_type=F32).astype(BF16).astype(F32)
            v = hg[3 + l, rows, own].astype(F32)
            t = gelu_tanh(v)
            slope = 0.5 * (1.0 + t) + (0.5 * v) * (1.0 - t * t) * (GELU_C * (1.0 + (3.0 * 0.044715) * (v * v)))
            hg[3 + l, rows, own] = (dh * slope).astype(BF16)

        share(3 + l).start()

    class Red:
        def __init__(self, first, width, acc, accx, s1, r1, r2, zr):
            self.first, self.width = first, width
            self.acc, self.accx, self.s1, self.r1, self.r2, self.zr = acc, accx, s1, r1, r2, zr

        def cols(self, j):
            return pl.ds(j * self.width, self.width)

        def st1(self, m, j):
            k = m - self.first
            return rcopy(self.s1.at[k, j], self.r1.at[k, j], s1_s.at[m, j], s1_r.at[m, j], (x_nbr, y_nbr)[j])

        def st2(self, m, j):
            k = m - self.first
            return rcopy(self.s1.at[k, 0, j], self.r2.at[k, j], s2_s.at[m, j], s2_r.at[m, j], (y_nbr, x_nbr)[j])

        def turn(self, m):
            k = m - self.first
            self.st1(m, 0).wait_send()
            for j in range(2):
                self.st1(m, j).wait_recv()
                put(self.s1, (k, 0, j), self.accx[k, j] + get(self.r1, (k, j, 1)))
                self.st2(m, j).start()
                self.acc[k, :, self.cols(j)] += get(self.r1, (k, j, 0))

        def z_copy(self, m):
            k = m - self.first
            kind = k // 4
            l = m % 4
            slot = (l - z + 3) % 4
            return rcopy(
                self.s1.at[k, 1], self.zr.at[kind, slot], z_s.at[m], z_r.at[m // 4, slot], (me + 8 * (l - z) + 32) % 32
            )

        def across(self, m):
            k = m - self.first
            self.st1(m, 1).wait_send()
            for j in range(2):
                self.st2(m, j).wait_recv()
                total = self.acc[k, :, self.cols(j)] + get(self.r2, (k, j))
                self.acc[k, :, self.cols(j)] = total

                @pl.when(m % 4 != z)
                def _():
                    put(self.s1, (k, 1, j), total)

            @pl.when(m % 4 != z)
            def _():
                self.z_copy(m).start()

        def z_wait(self, kind):
            for k in range(3):
                rcopy(
                    self.s1.at[0, 1], self.zr.at[kind, k], z_s.at[0], z_r.at[kind + self.first // 4, k], z_peer[k + 1]
                ).wait_recv()

        def z_total(self, kind, j):
            t = self.acc[kind * 4 + z, :, self.cols(j)]
            for k in range(3):
                t = t + get(self.zr, (kind, k, j))
            return t

    rg = Red(0, HALF, accg, accxg, s1g, r1g, r2g, zrg)
    rs = Red(4, BHALF, accs, accxs, s1s, r1s, r2s, zrs)

    def product(m):
        kind = m // 4
        l = m % 4
        left = jnp.where(kind == 2, 4 + l, l)
        right = jnp.where(kind == 1, l, 4 + l)
        for d in range(4):
            lhs[pl.ds(OWN * d, OWN), :] = hg[left, pl.ds(pl.multiple_of(blocks[d] * OWN, OWN), OWN), :]

        @pl.loop(0, 2)
        def _(j):
            cols = pl.ds(pl.multiple_of(j * HALF, HALF), HALF)
            full[:, cols] = lax.dot_general(lhs[...], hg[right, cols, :], NT, preferred_element_type=F32)

        def send(red, pieces):
            k = m - red.first
            for j in range(2):
                cols = slice(j * red.width, (j + 1) * red.width)
                near, other = (1, 2) if j == 0 else (2, 1)
                red.acc[k, :, cols] = pieces[0][:, cols]
                put(red.s1, (k, j, 0), pieces[near][:, cols])
                put(red.s1, (k, j, 1), pieces[3][:, cols])
                red.accx[k, j] = pieces[other][:, cols]
                red.st1(m, j).start()

        @pl.when(kind == 0)
        def _():
            send(rg, [full[pl.ds(OWN * d, OWN), :] for d in range(4)])

        @pl.when(kind > 0)
        def _():
            send(rs, [
                pltpu.roll(full[pl.ds(OWN * d, OWN), :], (D - OWN * blocks[d]) % D, 1)[:, :BAND] for d in range(4)
            ])

    def by_kind(name):
        def act(m):
            @pl.when(m < 4)
            def _():
                getattr(rg, name)(m)

            @pl.when(m >= 4)
            def _():
                getattr(rs, name)(m)

        return act

    inv_batch = 1.0 / BATCH

    def gather_copies(ref, base, ss, rs, own_src):
        def at(rb, half=None):
            return ref.at[base + rb] if half is None else ref.at[base + rb, half]

        first = [
            rcopy(own_src, at(blocks[0]), ss.at[0], rs.at[0], x_nbr),
            rcopy(own_src, at(blocks[0]), ss.at[1], rs.at[1], y_nbr),
            rcopy(own_src, at(blocks[0]), ss.at[2], rs.at[2], mate),
        ]
        from_x = [
            rcopy(at(blocks[1], 0), at(blocks[1], 0), ss.at[3], rs.at[3], y_nbr),
            rcopy(at(blocks[1]), at(blocks[1]), ss.at[5], rs.at[5], mate),
        ]
        from_y = [
            rcopy(at(blocks[2], 1), at(blocks[2], 1), ss.at[4], rs.at[4], x_nbr),
            rcopy(at(blocks[2]), at(blocks[2]), ss.at[6], rs.at[6], mate),
        ]
        last = rcopy(at(blocks[3]), at(blocks[3]), ss.at[7], rs.at[7], mate)
        return first, from_x, from_y, last

    def gather_rest(copies):
        first, from_x, from_y, last = copies
        first[0].wait_recv()
        for cp in from_x:
            cp.start()
        first[1].wait_recv()
        for cp in from_y:
            cp.start()

    def gather_last(copies):
        first, from_x, from_y, last = copies
        from_x[0].wait_recv()
        from_y[0].wait_recv()
        last.start()

    def gather_end(copies):
        first, from_x, from_y, last = copies
        for cp in (first[2], from_x[1], from_y[1], last):
            cp.wait_recv()

    def gather_sent(copies):
        first, from_x, from_y, last = copies
        for cp in (*first, *from_x, *from_y, last):
            cp.wait_send()

    g_copies = gather_copies(gcode, 0, g_s, g_r, gcode.at[blocks[0]])

    def u_row(l):
        return u_out.at[l * 8 + blocks[0]]

    def u_copies(k):
        l = (z - k + 4) % 4
        return gather_copies(u_out, l * 8, u_s.at[k], u_r.at[k], u_row(l))

    own_first = gather_copies(u_out, z * 8, u_s.at[0], u_r.at[0], ubuf)[0]
    local = pltpu.make_async_copy(ubuf, u_row(z), us_loc)

    def z_send(k, l):
        return rcopy(ubuf, u_row(l), uz_s.at[k - 1], uz_r.at[k - 1], (me + 8 * k) % 32)

    def own_grad(_):
        rg.z_wait(0)
        for j in range(2):
            put(gcode, (blocks[0], j), rg.z_total(0, j) * inv_batch)
        for cp in g_copies[0]:
            cp.start()

    def precondition(_):
        gather_end(g_copies)

        @pl.loop(0, 8)
        def _(b):
            for j in range(2):
                gfull[pl.ds(pl.multiple_of(b * OWN, OWN), OWN), pl.ds(j * HALF, HALF)] = get(gcode, (b, j))

        ld_si.wait()
        left_prod = jnp.dot(a_inv[...], gfull[...], precision=HIGH, preferred_element_type=F32)
        u_rows = jnp.dot(left_prod, sinv[...], precision=HIGH, preferred_element_type=F32)
        for j in range(2):
            put(ubuf, (j,), u_rows[:, j * HALF : (j + 1) * HALF])
        for k in range(1, 4):
            z_send(k, z).start()
        for cp in own_first:
            cp.start()
        local.start()

    def from_plane(k):
        z_send(k, (z - k + 4) % 4).wait_recv()
        for cp in u_copies(k)[0]:
            cp.start()

    def flip_copy(kind, e):
        return rcopy(
            flip.at[kind, e - 1], f_flip.at[kind, e - 1], t_s.at[kind, e - 1], t_r.at[kind, e - 1],
            z * 8 + (blocks[0] + e) % 8,
        )

    def factors(_):
        for kind in range(2):
            rs.z_wait(kind)
            for j in range(2):
                f_sum[kind, :, rs.cols(j)] = rs.z_total(kind, j)
            turned = f_sum[kind].T
            for e in range(1, 4):
                flip[kind, e - 1, :, pl.ds(0, OWN)] = turned[OWN * e : OWN * (e + 1)]
                flip_copy(kind, e).start()

    def factors_end():
        for kind in range(2):
            for e in range(1, 4):
                flip_copy(kind, e).wait()

    def turn_rows(k, n):
        for i in range(8):
            for j in range(2):
                piece(k, i, j).wait()
                hg[n, pl.ds(j * HALF, HALF), pl.ds(i * 128, 128)] = stage(i, j, k)[...].T

        share(n).start()

    turn_rows(0, 0)

    actions = {
        F: forward,
        B: backward,
        W: lambda n: share(n).wait_recv(),
        PR: product,
        T: by_kind("turn"),
        C: by_kind("across"),
        Z: own_grad,
        R: lambda _: gather_rest(g_copies),
        U: precondition,
        Y: from_plane,
        V: lambda k: gather_rest(u_copies(k)),
        AS: factors,
        RQ: lambda _: gather_last(g_copies),
        VQ: lambda k: gather_last(u_copies(k)),
        DY: lambda _: turn_rows(1, 7),
    }

    @pl.loop(0, len(EVENTS))
    def _(step):
        code = jnp.int32(0)
        for s, (op, arg) in enumerate(EVENTS):
            code = jnp.where(step == s, op * 16 + arg, code)
        op = code // 16
        arg = code % 16
        for o, act in actions.items():

            @pl.when(op == o)
            def _(act=act):
                act(arg)

    @pl.loop(0, 4)
    def _(k):
        gather_end(u_copies(k))
        gather_sent(u_copies(k))

    for k in range(1, 4):
        z_send(k, z).wait_send()
    local.wait()
    gather_sent(g_copies)

    @pl.loop(0, 8)
    def _(n):
        share(n).wait_send()

    factors_end()

    @pl.loop(0, 12)
    def _(m):
        def sent(red):
            for j in range(2):
                red.st2(m, j).wait_send()

            @pl.when(m % 4 != z)
            def _():
                red.z_copy(m).wait_send()

        @pl.when(m < 4)
        def _():
            sent(rg)

        @pl.when(m >= 4)
        def _():
            sent(rs)


PARTS = 8
PER = LAYERS * 8 // PARTS


def finish(code_hbm, a_old, s_old, f_sum, f_flip, rows_hbm, a_new, s_new, code, rows, old, tot, flip, in_sem, out_sem, f_sem):
    def load(i):
        return pltpu.make_async_copy(code_hbm.at[pl.ds(i * PER, PER)], code.at[pl.ds(i * PER, PER)], in_sem.at[i])

    def store(i):
        part = pl.ds(pl.multiple_of(i * PER * OWN, OWN), PER * OWN)
        return pltpu.make_async_copy(rows.at[part], rows_hbm.at[part], out_sem.at[i])

    pairs = ((a_old, a_new), (s_old, s_new))
    moves = [pltpu.make_async_copy(o, old.at[k], f_sem.at[k]) for k, (o, _) in enumerate(pairs)]
    moves.append(pltpu.make_async_copy(f_sum, tot.at[:, :, pl.ds(0, BAND)], f_sem.at[2]))
    moves.append(pltpu.make_async_copy(f_flip, flip, f_sem.at[3]))
    outs = [pltpu.make_async_copy(old.at[k], n, f_sem.at[4 + k]) for k, (_, n) in enumerate(pairs)]
    for cp in moves:
        cp.start()
    for i in range(PARTS):
        load(i).start()
    for cp in moves:
        cp.wait()
    shift = OWN * (lax.axis_index("data") % 8)
    for k in range(2):
        for e in range(1, 4):
            at = D - OWN * e
            tot[k, :, at : at + OWN] = flip[k, e - 1, :, 0:OWN]
        old[k] = DECAY * old[k] + ((1.0 - DECAY) / BATCH) * pltpu.roll(tot[k], shift, 1)
        outs[k].start()

    @pl.loop(0, PARTS)
    def _(i):
        load(i).wait()
        for b in range(PER):
            n = i * PER + b
            for j in range(2):
                rows[pl.ds(pl.multiple_of(n * OWN, OWN), OWN), pl.ds(j * HALF, HALF)] = get(code, (n, j))
        store(i).start()

    for cp in outs:
        cp.wait()
    for i in range(PARTS):
        store(i).wait()


def solution(mesh):
    def device_step(x_loc, dy_loc, weights, a_old_rows, s_old_rows, a_inv_rows, s_inv):
        hbm = pl.BlockSpec(memory_space=pltpu.HBM)
        vmem = pl.BlockSpec(memory_space=pltpu.VMEM)
        dma = pltpu.SemaphoreType.DMA
        u_code, f_sum, f_flip = pl.pallas_call(
            kernel,
            out_shape=(
                jax.ShapeDtypeStruct((LAYERS * 8, 2, CODE, HALF), BF16),
                jax.ShapeDtypeStruct((2, OWN, BAND), F32),
                jax.ShapeDtypeStruct((2, 3, OWN, 128), F32),
            ),
            in_specs=[hbm] * 4 + [vmem],
            out_specs=(hbm, vmem, hbm),
            scratch_shapes=[
                pltpu.VMEM((2 * LAYERS, D, 2 * ROWS), BF16),
                pltpu.VMEM((3, D, D), BF16),
                pltpu.VMEM((4 * OWN, 2 * ROWS), BF16),
                pltpu.VMEM((4 * OWN, D), F32),
                pltpu.VMEM((4, OWN, D), F32),
                pltpu.VMEM((4, 2, OWN, HALF), F32),
                pltpu.VMEM((4, 2, 2, CODE, HALF), BF16),
                pltpu.VMEM((4, 2, 2, CODE, HALF), BF16),
                pltpu.VMEM((4, 2, CODE, HALF), BF16),
                pltpu.VMEM((1, 3, 2, CODE, HALF), BF16),
                pltpu.VMEM((8, OWN, BAND), F32),
                pltpu.VMEM((8, 2, OWN, BHALF), F32),
                pltpu.VMEM((8, 2, 2, CODE, BHALF), BF16),
                pltpu.VMEM((8, 2, 2, CODE, BHALF), BF16),
                pltpu.VMEM((8, 2, CODE, BHALF), BF16),
                pltpu.VMEM((2, 3, 2, CODE, BHALF), BF16),
                pltpu.VMEM((2, 3, OWN, 128), F32),
                pltpu.VMEM((8, 2, CODE, HALF), BF16),
                pltpu.VMEM((D, D), F32),
                pltpu.VMEM((D, D), F32),
                pltpu.VMEM((2, CODE, HALF), BF16),
                dma((2, 8, 2)),
                dma,
                dma((3,)),
                dma((8,)), dma((8,)),
                dma((12, 2)), dma((12, 2)),
                dma((12, 2)), dma((12, 2)),
                dma((12,)), dma((3, 3)),
                dma((2, 3)), dma((2, 3)),
                dma((8,)), dma((8,)),
                dma((3,)), dma((3,)),
                dma((4, 8)), dma((4, 8)),
                dma,
            ],
            compiler_params=pltpu.CompilerParams(
                collective_id=0, has_side_effects=True, vmem_limit_bytes=67_000_000
            ),
        )(x_loc, dy_loc, weights, s_inv, a_inv_rows)
        own_shape = jax.ShapeDtypeStruct((OWN, D), F32)
        u_rows, a_new, s_new = pl.pallas_call(
            finish,
            out_shape=(jax.ShapeDtypeStruct((LAYERS * D, D), F32), own_shape, own_shape),
            in_specs=[hbm] * 5,
            out_specs=(hbm, hbm, hbm),
            scratch_shapes=[
                pltpu.VMEM((LAYERS * 8, 2, CODE, HALF), BF16),
                pltpu.VMEM((LAYERS * D, D), F32),
                pltpu.VMEM((2, OWN, D), F32),
                pltpu.VMEM((2, OWN, D), F32),
                pltpu.VMEM((2, 3, OWN, 128), F32),
                dma((PARTS,)),
                dma((PARTS,)),
                dma((6,)),
            ],
            compiler_params=pltpu.CompilerParams(vmem_limit_bytes=67_000_000),
        )(u_code, a_old_rows, s_old_rows, f_sum, f_flip)
        return u_rows.reshape(LAYERS, D, D), a_new, s_new

    row_spec = P("data", None)
    return jax.shard_map(
        device_step,
        mesh=mesh,
        in_specs=(row_spec, row_spec, P(), row_spec, row_spec, row_spec, P()),
        out_specs=(P(), row_spec, row_spec),
        check_vma=False,
    )
```

```python
import math
import jax
import jax.numpy as jnp
from jax import lax
from jax.experimental import pallas as pl
from jax.experimental.pallas import tpu as pltpu
from jax.sharding import PartitionSpec as P

DECAY = 0.75
F32 = jnp.float32
BF16 = jnp.bfloat16
MESH = pl.DeviceIdType.MESH
HIGH = lax.Precision.HIGHEST
LAYERS = 4
D = 768
ROWS = 1024
BATCH = 32 * ROWS
OWN = 96
HALF = 384
BAND = 512
BHALF = BAND // 2
GELU_C = math.sqrt(2.0 / math.pi)
NT = (((1,), (1,)), ((), ()))
TN = (((0,), (0,)), ((), ()))

STEPS = 2560.0
BASE = 21.0
PAIR = OWN // 2
CODE = OWN + PAIR


def nearest(v):
    return (v + 12582912.0) - 12582912.0


def encode(v):
    hi = v.astype(BF16)
    h = hi.astype(F32)
    q = nearest(jnp.clip((v - h) / jnp.where(h == 0.0, 1.0, h) * STEPS, -10.0, 10.0))
    lo = q[:PAIR] * BASE + q[PAIR:]
    return hi, lo.astype(BF16)


def decode(hi, lo):
    h = hi.astype(F32)
    w = lo.astype(F32)
    top = nearest(w * (1.0 / BASE))
    q = jnp.concatenate([top, w - BASE * top], axis=-2)
    return h + h * (q * (1.0 / STEPS))


def put(ref, idx, v):
    hi, lo = encode(v)
    ref[(*idx, slice(0, OWN))] = hi
    ref[(*idx, slice(OWN, CODE))] = lo


def get(ref, idx):
    return decode(ref[(*idx, slice(0, OWN))], ref[(*idx, slice(OWN, CODE))])


def gelu_tanh(v):
    return jnp.tanh(GELU_C * (v + 0.044715 * (v * v * v)))


F, B, W, PR, T, C, Z, R, U, Y, V, AS, RQ, VQ, DY = range(15)
EVENTS = [
    (F, 0), (DY, 0), (F, 1), (F, 2), (W, 7), (PR, 11), (B, 3), (W, 3), (PR, 3), (B, 2),
    (W, 2), (W, 6), (PR, 2), (B, 1), (T, 11), (T, 3), (T, 2), (W, 0), (W, 4), (PR, 0),
    (C, 3), (PR, 6), (T, 0), (W, 1), (W, 5), (PR, 1), (PR, 5), (C, 0), (C, 2), (T, 1),
    (PR, 9), (T, 5), (C, 1), (PR, 7), (C, 11), (PR, 10), (Z, 0), (R, 0), (PR, 4), (C, 5),
    (T, 6), (T, 10), (RQ, 0), (T, 7), (U, 0), (PR, 8), (V, 0), (T, 9), (T, 8), (T, 4),
    (Y, 3), (C, 4), (C, 6), (Y, 2), (V, 3), (C, 10), (VQ, 0), (Y, 1), (C, 7), (C, 8),
    (V, 2), (C, 9), (V, 1), (VQ, 1), (VQ, 3), (VQ, 2), (AS, 0),
]


def kernel(
    x_hbm, dy_hbm, w_hbm, sinv_hbm, a_inv,
    u_out, f_sum, f_flip,
    hg, wbuf, lhs, full, accg, accxg, s1g, r1g, r2g, zrg, accs, accxs, s1s, r1s, r2s, zrs, flip, gcode, gfull, sinv, ubuf,
    in_sem, lsem, wsem, d2d_s, d2d_r, s1_s, s1_r, s2_s, s2_r, z_s, z_r, t_s, t_r, g_s, g_r, uz_s, uz_r, u_s, u_r, us_loc,
):
    me = lax.axis_index("data")
    c = me % 2
    x = (me // 2) % 2
    y = (me // 4) % 2
    z = me // 8
    mate = me + 1 - 2 * c
    x_nbr = me + 2 - 4 * x
    y_nbr = me + 4 - 8 * y
    z_peer = [(me + 8 * k) % 32 for k in range(4)]

    def row_block(dy_, dx_):
        return 4 * ((y + dy_) % 2) + 2 * ((x + dx_) % 2) + c

    blocks = [row_block(0, 0), row_block(0, 1), row_block(1, 0), row_block(1, 1)]

    def rcopy(src, dst, ss, rs, dev):
        return pltpu.make_async_remote_copy(
            src_ref=src, dst_ref=dst, send_sem=ss, recv_sem=rs, device_id=(dev,), device_id_type=MESH
        )

    own = pl.ds(0, ROWS)
    far = pl.ds(ROWS, ROWS)
    def stage(i, j, k):
        return (s1g.at[i, j, k] if i < 4 else gcode.at[2 * (i - 4) + k, j]).at[pl.ds(0, 128)]

    def piece(k, i, j):
        src = (x_hbm, dy_hbm)[k].at[pl.ds(128 * i, 128), pl.ds(HALF * j, HALF)]
        return pltpu.make_async_copy(src, stage(i, j, k), in_sem.at[k, i, j])

    ld_si = pltpu.make_async_copy(sinv_hbm.at[z], sinv, lsem)
    for k in range(2):
        for i in range(8):
            for j in range(2):
                piece(k, i, j).start()
    for l in range(3):
        pltpu.make_async_copy(w_hbm.at[l], wbuf.at[l], wsem.at[l]).start()
    ld_si.start()

    barrier = pltpu.get_barrier_semaphore()
    for dev in [z * 8 + (me + k) % 8 for k in range(1, 8)] + z_peer[1:]:
        pl.semaphore_signal(barrier, inc=1, device_id=(dev,), device_id_type=MESH)
    pl.semaphore_wait(barrier, 10)

    def share(n):
        return rcopy(hg.at[n, :, own], hg.at[n, :, far], d2d_s.at[n], d2d_r.at[n], mate)

    def forward(l):
        pltpu.make_async_copy(w_hbm.at[l], wbuf.at[l], wsem.at[l]).wait()

        @pl.loop(0, 3)
        def _(i):
            rows = pl.ds(pl.multiple_of(i * 256, 256), 256)
            pre = lax.dot_general(wbuf[l, :, rows], hg[l, :, own], TN, preferred_element_type=F32).astype(BF16)
            hg[4 + l, rows, own] = pre
            v = pre.astype(F32)
            hg[l + 1, rows, own] = (v * (0.5 * (1.0 + gelu_tanh(v)))).astype(BF16)

        share(l + 1).start()

        @pl.when(l == 0)
        def _():
            pltpu.make_async_copy(w_hbm.at[3], wbuf.at[0], wsem.at[0]).start()

    def backward(l):
        k = l % 3

        @pl.when(l == 3)
        def _():
            pltpu.make_async_copy(w_hbm.at[3], wbuf.at[0], wsem.at[0]).wait()

        @pl.loop(0, 3)
        def _(i):
            rows = pl.ds(pl.multiple_of(i * 256, 256), 256)
            dh = jnp.dot(wbuf[k, rows, :], hg[4 + l, :, own], preferred_element_type=F32).astype(BF16).astype(F32)
            v = hg[3 + l, rows, own].astype(F32)
            t = gelu_tanh(v)
            slope = 0.5 * (1.0 + t) + (0.5 * v) * (1.0 - t * t) * (GELU_C * (1.0 + (3.0 * 0.044715) * (v * v)))
            hg[3 + l, rows, own] = (dh * slope).astype(BF16)

        share(3 + l).start()

    class Red:
        def __init__(self, first, width, acc, accx, s1, r1, r2, zr):
            self.first, self.width = first, width
            self.acc, self.accx, self.s1, self.r1, self.r2, self.zr = acc, accx, s1, r1, r2, zr

        def cols(self, j):
            return pl.ds(j * self.width, self.width)

        def st1(self, m, j):
            k = m - self.first
            return rcopy(self.s1.at[k, j], self.r1.at[k, j], s1_s.at[m, j], s1_r.at[m, j], (x_nbr, y_nbr)[j])

        def st2(self, m, j):
            k = m - self.first
            return rcopy(self.s1.at[k, 0, j], self.r2.at[k, j], s2_s.at[m, j], s2_r.at[m, j], (y_nbr, x_nbr)[j])

        def turn(self, m):
            k = m - self.first
            self.st1(m, 0).wait_send()
            for j in range(2):
                self.st1(m, j).wait_recv()
                put(self.s1, (k, 0, j), self.accx[k, j] + get(self.r1, (k, j, 1)))
                self.st2(m, j).start()
                self.acc[k, :, self.cols(j)] += get(self.r1, (k, j, 0))

        def z_copy(self, m):
            k = m - self.first
            kind = k // 4
            l = m % 4
            slot = (l - z + 3) % 4
            return rcopy(
                self.s1.at[k, 1], self.zr.at[kind, slot], z_s.at[m], z_r.at[m // 4, slot], (me + 8 * (l - z) + 32) % 32
            )

        def across(self, m):
            k = m - self.first
            self.st1(m, 1).wait_send()
            for j in range(2):
                self.st2(m, j).wait_recv()
                total = self.acc[k, :, self.cols(j)] + get(self.r2, (k, j))
                self.acc[k, :, self.cols(j)] = total

                @pl.when(m % 4 != z)
                def _():
                    put(self.s1, (k, 1, j), total)

            @pl.when(m % 4 != z)
            def _():
                self.z_copy(m).start()

        def z_wait(self, kind):
            for k in range(3):
                rcopy(
                    self.s1.at[0, 1], self.zr.at[kind, k], z_s.at[0], z_r.at[kind + self.first // 4, k], z_peer[k + 1]
                ).wait_recv()

        def z_total(self, kind, j):
            t = self.acc[kind * 4 + z, :, self.cols(j)]
            for k in range(3):
                t = t + get(self.zr, (kind, k, j))
            return t

    rg = Red(0, HALF, accg, accxg, s1g, r1g, r2g, zrg)
    rs = Red(4, BHALF, accs, accxs, s1s, r1s, r2s, zrs)

    def product(m):
        kind = m // 4
        l = m % 4
        left = jnp.where(kind == 2, 4 + l, l)
        right = jnp.where(kind == 1, l, 4 + l)
        for d in range(4):
            lhs[pl.ds(OWN * d, OWN), :] = hg[left, pl.ds(pl.multiple_of(blocks[d] * OWN, OWN), OWN), :]

        @pl.loop(0, 2)
        def _(j):
            cols = pl.ds(pl.multiple_of(j * HALF, HALF), HALF)
            full[:, cols] = lax.dot_general(lhs[...], hg[right, cols, :], NT, preferred_element_type=F32)

        def send(red, pieces):
            k = m - red.first
            for j in range(2):
                cols = slice(j * red.width, (j + 1) * red.width)
                near, other = (1, 2) if j == 0 else (2, 1)
                red.acc[k, :, cols] = pieces[0][:, cols]
                put(red.s1, (k, j, 0), pieces[near][:, cols])
                put(red.s1, (k, j, 1), pieces[3][:, cols])
                red.accx[k, j] = pieces[other][:, cols]
                red.st1(m, j).start()

        @pl.when(kind == 0)
        def _():
            send(rg, [full[pl.ds(OWN * d, OWN), :] for d in range(4)])

        @pl.when(kind > 0)
        def _():
            send(rs, [
                pltpu.roll(full[pl.ds(OWN * d, OWN), :], (D - OWN * blocks[d]) % D, 1)[:, :BAND] for d in range(4)
            ])

    def by_kind(name):
        def act(m):
            @pl.when(m < 4)
            def _():
                getattr(rg, name)(m)

            @pl.when(m >= 4)
            def _():
                getattr(rs, name)(m)

        return act

    inv_batch = 1.0 / BATCH

    def gather_copies(ref, base, ss, rs, own_src):
        def at(rb, half=None):
            return ref.at[base + rb] if half is None else ref.at[base + rb, half]

        first = [
            rcopy(own_src, at(blocks[0]), ss.at[0], rs.at[0], x_nbr),
            rcopy(own_src, at(blocks[0]), ss.at[1], rs.at[1], y_nbr),
            rcopy(own_src, at(blocks[0]), ss.at[2], rs.at[2], mate),
        ]
        from_x = [
            rcopy(at(blocks[1], 0), at(blocks[1], 0), ss.at[3], rs.at[3], y_nbr),
            rcopy(at(blocks[1]), at(blocks[1]), ss.at[5], rs.at[5], mate),
        ]
        from_y = [
            rcopy(at(blocks[2], 1), at(blocks[2], 1), ss.at[4], rs.at[4], x_nbr),
            rcopy(at(blocks[2]), at(blocks[2]), ss.at[6], rs.at[6], mate),
        ]
        last = rcopy(at(blocks[3]), at(blocks[3]), ss.at[7], rs.at[7], mate)
        return first, from_x, from_y, last

    def gather_rest(copies):
        first, from_x, from_y, last = copies
        first[0].wait_recv()
        for cp in from_x:
            cp.start()
        first[1].wait_recv()
        for cp in from_y:
            cp.start()

    def gather_last(copies):
        first, from_x, from_y, last = copies
        from_x[0].wait_recv()
        from_y[0].wait_recv()
        last.start()

    def gather_end(copies):
        first, from_x, from_y, last = copies
        for cp in (first[2], from_x[1], from_y[1], last):
            cp.wait_recv()

    def gather_sent(copies):
        first, from_x, from_y, last = copies
        for cp in (*first, *from_x, *from_y, last):
            cp.wait_send()

    g_copies = gather_copies(gcode, 0, g_s, g_r, gcode.at[blocks[0]])

    def u_row(l):
        return u_out.at[l * 8 + blocks[0]]

    def u_copies(k):
        l = (z - k + 4) % 4
        return gather_copies(u_out, l * 8, u_s.at[k], u_r.at[k], u_row(l))

    own_first = gather_copies(u_out, z * 8, u_s.at[0], u_r.at[0], ubuf)[0]
    local = pltpu.make_async_copy(ubuf, u_row(z), us_loc)

    def z_send(k, l):
        return rcopy(ubuf, u_row(l), uz_s.at[k - 1], uz_r.at[k - 1], (me + 8 * k) % 32)

    def own_grad(_):
        rg.z_wait(0)
        for j in range(2):
            put(gcode, (blocks[0], j), rg.z_total(0, j) * inv_batch)
        for cp in g_copies[0]:
            cp.start()

    def precondition(_):
        gather_end(g_copies)

        @pl.loop(0, 8)
        def _(b):
            for j in range(2):
                gfull[pl.ds(pl.multiple_of(b * OWN, OWN), OWN), pl.ds(j * HALF, HALF)] = get(gcode, (b, j))

        ld_si.wait()
        left_prod = jnp.dot(a_inv[...], gfull[...], precision=HIGH, preferred_element_type=F32)
        u_rows = jnp.dot(left_prod, sinv[...], precision=HIGH, preferred_element_type=F32)
        for j in range(2):
            put(ubuf, (j,), u_rows[:, j * HALF : (j + 1) * HALF])
        for k in range(1, 4):
            z_send(k, z).start()
        for cp in own_first:
            cp.start()
        local.start()

    def from_plane(k):
        z_send(k, (z - k + 4) % 4).wait_recv()
        for cp in u_copies(k)[0]:
            cp.start()

    def flip_copy(kind, e):
        return rcopy(
            flip.at[kind, e - 1], f_flip.at[kind, e - 1], t_s.at[kind, e - 1], t_r.at[kind, e - 1],
            z * 8 + (blocks[0] + e) % 8,
        )

    def factors(_):
        for kind in range(2):
            rs.z_wait(kind)
            for j in range(2):
                f_sum[kind, :, rs.cols(j)] = rs.z_total(kind, j)
            turned = f_sum[kind].T
            for e in range(1, 4):
                flip[kind, e - 1, :, pl.ds(0, OWN)] = turned[OWN * e : OWN * (e + 1)]
                flip_copy(kind, e).start()

    def factors_end():
        for kind in range(2):
            for e in range(1, 4):
                flip_copy(kind, e).wait()

    def turn_rows(k, n):
        for i in range(8):
            for j in range(2):
                piece(k, i, j).wait()
                hg[n, pl.ds(j * HALF, HALF), pl.ds(i * 128, 128)] = stage(i, j, k)[...].T

        share(n).start()

    turn_rows(0, 0)

    actions = {
        F: forward,
        B: backward,
        W: lambda n: share(n).wait_recv(),
        PR: product,
        T: by_kind("turn"),
        C: by_kind("across"),
        Z: own_grad,
        R: lambda _: gather_rest(g_copies),
        U: precondition,
        Y: from_plane,
        V: lambda k: gather_rest(u_copies(k)),
        AS: factors,
        RQ: lambda _: gather_last(g_copies),
        VQ: lambda k: gather_last(u_copies(k)),
        DY: lambda _: turn_rows(1, 7),
    }

    @pl.loop(0, len(EVENTS))
    def _(step):
        code = jnp.int32(0)
        for s, (op, arg) in enumerate(EVENTS):
            code = jnp.where(step == s, op * 16 + arg, code)
        op = code // 16
        arg = code % 16
        for o, act in actions.items():

            @pl.when(op == o)
            def _(act=act):
                act(arg)

    @pl.loop(0, 4)
    def _(k):
        gather_end(u_copies(k))
        gather_sent(u_copies(k))

    for k in range(1, 4):
        z_send(k, z).wait_send()
    local.wait()
    gather_sent(g_copies)

    @pl.loop(0, 8)
    def _(n):
        share(n).wait_send()

    factors_end()

    @pl.loop(0, 12)
    def _(m):
        def sent(red):
            for j in range(2):
                red.st2(m, j).wait_send()

            @pl.when(m % 4 != z)
            def _():
                red.z_copy(m).wait_send()

        @pl.when(m < 4)
        def _():
            sent(rg)

        @pl.when(m >= 4)
        def _():
            sent(rs)


PARTS = 8
PER = LAYERS * 8 // PARTS


def finish(code_hbm, a_old, s_old, f_sum, f_flip, rows_hbm, a_new, s_new, code, rows, old, tot, flip, in_sem, out_sem, f_sem):
    def load(i):
        return pltpu.make_async_copy(code_hbm.at[pl.ds(i * PER, PER)], code.at[pl.ds(i * PER, PER)], in_sem.at[i])

    def store(i):
        part = pl.ds(pl.multiple_of(i * PER * OWN, OWN), PER * OWN)
        return pltpu.make_async_copy(rows.at[part], rows_hbm.at[part], out_sem.at[i])

    pairs = ((a_old, a_new), (s_old, s_new))
    moves = [pltpu.make_async_copy(o, old.at[k], f_sem.at[k]) for k, (o, _) in enumerate(pairs)]
    moves.append(pltpu.make_async_copy(f_sum, tot.at[:, :, pl.ds(0, BAND)], f_sem.at[2]))
    moves.append(pltpu.make_async_copy(f_flip, flip, f_sem.at[3]))
    outs = [pltpu.make_async_copy(old.at[k], n, f_sem.at[4 + k]) for k, (_, n) in enumerate(pairs)]
    for cp in moves:
        cp.start()
    for i in range(PARTS):
        load(i).start()
    for cp in moves:
        cp.wait()
    shift = OWN * (lax.axis_index("data") % 8)
    for k in range(2):
        for e in range(1, 4):
            at = D - OWN * e
            tot[k, :, at : at + OWN] = flip[k, e - 1, :, 0:OWN]
        old[k] = DECAY * old[k] + ((1.0 - DECAY) / BATCH) * pltpu.roll(tot[k], shift, 1)
        outs[k].start()

    @pl.loop(0, PARTS)
    def _(i):
        load(i).wait()
        for b in range(PER):
            n = i * PER + b
            for j in range(2):
                rows[pl.ds(pl.multiple_of(n * OWN, OWN), OWN), pl.ds(j * HALF, HALF)] = get(code, (n, j))
        store(i).start()

    for cp in outs:
        cp.wait()
    for i in range(PARTS):
        store(i).wait()


def solution(mesh):
    def device_step(x_loc, dy_loc, weights, a_old_rows, s_old_rows, a_inv_rows, s_inv):
        hbm = pl.BlockSpec(memory_space=pltpu.HBM)
        vmem = pl.BlockSpec(memory_space=pltpu.VMEM)
        dma = pltpu.SemaphoreType.DMA
        u_code, f_sum, f_flip = pl.pallas_call(
            kernel,
            out_shape=(
                jax.ShapeDtypeStruct((LAYERS * 8, 2, CODE, HALF), BF16),
                jax.ShapeDtypeStruct((2, OWN, BAND), F32),
                jax.ShapeDtypeStruct((2, 3, OWN, 128), F32),
            ),
            in_specs=[hbm] * 4 + [vmem],
            out_specs=(hbm, vmem, hbm),
            scratch_shapes=[
                pltpu.VMEM((2 * LAYERS, D, 2 * ROWS), BF16),
                pltpu.VMEM((3, D, D), BF16),
                pltpu.VMEM((4 * OWN, 2 * ROWS), BF16),
                pltpu.VMEM((4 * OWN, D), F32),
                pltpu.VMEM((4, OWN, D), F32),
                pltpu.VMEM((4, 2, OWN, HALF), F32),
                pltpu.VMEM((4, 2, 2, CODE, HALF), BF16),
                pltpu.VMEM((4, 2, 2, CODE, HALF), BF16),
                pltpu.VMEM((4, 2, CODE, HALF), BF16),
                pltpu.VMEM((1, 3, 2, CODE, HALF), BF16),
                pltpu.VMEM((8, OWN, BAND), F32),
                pltpu.VMEM((8, 2, OWN, BHALF), F32),
                pltpu.VMEM((8, 2, 2, CODE, BHALF), BF16),
                pltpu.VMEM((8, 2, 2, CODE, BHALF), BF16),
                pltpu.VMEM((8, 2, CODE, BHALF), BF16),
                pltpu.VMEM((2, 3, 2, CODE, BHALF), BF16),
                pltpu.VMEM((2, 3, OWN, 128), F32),
                pltpu.VMEM((8, 2, CODE, HALF), BF16),
                pltpu.VMEM((D, D), F32),
                pltpu.VMEM((D, D), F32),
                pltpu.VMEM((2, CODE, HALF), BF16),
                dma((2, 8, 2)),
                dma,
                dma((3,)),
                dma((8,)), dma((8,)),
                dma((12, 2)), dma((12, 2)),
                dma((12, 2)), dma((12, 2)),
                dma((12,)), dma((3, 3)),
                dma((2, 3)), dma((2, 3)),
                dma((8,)), dma((8,)),
                dma((3,)), dma((3,)),
                dma((4, 8)), dma((4, 8)),
                dma,
            ],
            compiler_params=pltpu.CompilerParams(
                collective_id=0, has_side_effects=True, vmem_limit_bytes=67_000_000
            ),
        )(x_loc, dy_loc, weights, s_inv, a_inv_rows)
        own_shape = jax.ShapeDtypeStruct((OWN, D), F32)
        u_rows, a_new, s_new = pl.pallas_call(
            finish,
            out_shape=(jax.ShapeDtypeStruct((LAYERS * D, D), F32), own_shape, own_shape),
            in_specs=[hbm] * 5,
            out_specs=(hbm, hbm, hbm),
            scratch_shapes=[
                pltpu.VMEM((LAYERS * 8, 2, CODE, HALF), BF16),
                pltpu.VMEM((LAYERS * D, D), F32),
                pltpu.VMEM((2, OWN, D), F32),
                pltpu.VMEM((2, OWN, D), F32),
                pltpu.VMEM((2, 3, OWN, 128), F32),
                dma((PARTS,)),
                dma((PARTS,)),
                dma((6,)),
            ],
            compiler_params=pltpu.CompilerParams(vmem_limit_bytes=67_000_000),
        )(u_code, a_old_rows, s_old_rows, f_sum, f_flip)
        return u_rows.reshape(LAYERS, D, D), a_new, s_new

    row_spec = P("data", None)
    return jax.shard_map(
        device_step,
        mesh=mesh,
        in_specs=(row_spec, row_spec, P(), row_spec, row_spec, row_spec, P()),
        out_specs=(P(), row_spec, row_spec),
        check_vma=False,
    )
```

```python
import math
import jax
import jax.numpy as jnp
from jax import lax
from jax.experimental import pallas as pl
from jax.experimental.pallas import tpu as pltpu
from jax.sharding import PartitionSpec as P

DECAY = 0.75
F32 = jnp.float32
BF16 = jnp.bfloat16
MESH = pl.DeviceIdType.MESH
HIGH = lax.Precision.HIGHEST
LAYERS = 4
D = 768
ROWS = 1024
BATCH = 32 * ROWS
OWN = 96
HALF = 384
BAND = 512
BHALF = BAND // 2
GELU_C = math.sqrt(2.0 / math.pi)
NT = (((1,), (1,)), ((), ()))
TN = (((0,), (0,)), ((), ()))

STEPS = {2: 2560.0, 3: 768.0}
BASE = {2: 21.0, 3: 7.0}
CODE = OWN + OWN // 2
SCODE = OWN + OWN // 3


def nearest(v):
    return (v + 12582912.0) - 12582912.0


def encode(v, group):
    hi = v.astype(BF16)
    h = hi.astype(F32)
    bound = STEPS[group] / 256.0
    q = nearest(jnp.clip((v - h) / jnp.where(h == 0.0, 1.0, h) * STEPS[group], -bound, bound))
    n = OWN // group
    word = q[:n]
    for k in range(1, group):
        word = word * BASE[group] + q[k * n : (k + 1) * n]
    return hi, word.astype(BF16)


def decode(hi, lo, group):
    h = hi.astype(F32)
    w = lo.astype(F32)
    parts = []
    for k in range(group - 1, 0, -1):
        unit = BASE[group] ** k
        parts.append(nearest(w * (1.0 / unit)))
        w = w - unit * parts[-1]
    q = jnp.concatenate([*parts, w], axis=-2)
    return h + h * (q * (1.0 / STEPS[group]))


def rows_of(ref):
    return ref.shape[-2], OWN // (ref.shape[-2] - OWN)


def put(ref, idx, v):
    rows, group = rows_of(ref)
    hi, lo = encode(v, group)
    ref[(*idx, slice(0, OWN))] = hi
    ref[(*idx, slice(OWN, rows))] = lo


def get(ref, idx):
    rows, group = rows_of(ref)
    return decode(ref[(*idx, slice(0, OWN))], ref[(*idx, slice(OWN, rows))], group)


def gelu_tanh(v):
    return jnp.tanh(GELU_C * (v + 0.044715 * (v * v * v)))


F, B, W, PR, T, C, Z, R, U, Y, V, AS, RQ, VQ, DY = range(15)
EVENTS = [
    (F, 0), (DY, 0), (F, 1), (F, 2), (W, 7), (PR, 11), (B, 3), (W, 3), (PR, 3), (B, 2),
    (W, 2), (W, 6), (PR, 2), (B, 1), (W, 1), (W, 5), (PR, 1), (W, 0), (W, 4), (PR, 0),
    (T, 1), (T, 3), (PR, 5), (T, 0), (C, 1), (T, 2), (PR, 10), (C, 3), (PR, 6), (C, 0),
    (PR, 7), (PR, 9), (T, 5), (T, 11), (C, 2), (Z, 0), (R, 0), (C, 5), (PR, 8), (T, 7),
    (RQ, 0), (C, 11), (T, 9), (T, 6), (U, 0), (PR, 4), (T, 8), (V, 0), (T, 4), (C, 6),
    (T, 10), (Y, 1), (C, 9), (Y, 2), (C, 4), (V, 1), (C, 8), (Y, 3), (C, 10), (V, 2),
    (C, 7), (VQ, 0), (V, 3), (VQ, 1), (VQ, 2), (AS, 0), (VQ, 3),
]
CODES = [op * 16 + arg for op, arg in EVENTS]
CODES += [0] * (-len(CODES) % 3)
PLAN = [a + 256 * b + 65536 * c for a, b, c in zip(CODES[::3], CODES[1::3], CODES[2::3])]


def kernel(
    x_hbm, dy_hbm, w_hbm, sinv_hbm, a_inv,
    u_out, f_sum, f_flip,
    hg, wbuf, lhs, full, accg, accxg, s1g, r1g, r2g, zrg, accs, accxs, s1s, r1s, r2s, zrs, flip, gcode, gfull, sinv, ubuf,
    in_sem, lsem, wsem, d2d_s, d2d_r, s1_s, s1_r, s2_s, s2_r, z_s, z_r, t_s, t_r, g_s, g_r, uz_s, uz_r, u_s, u_r, us_loc,
):
    me = lax.axis_index("data")
    c = me % 2
    x = (me // 2) % 2
    y = (me // 4) % 2
    z = me // 8
    mate = me + 1 - 2 * c
    x_nbr = me + 2 - 4 * x
    y_nbr = me + 4 - 8 * y
    z_peer = [(me + 8 * k) % 32 for k in range(4)]

    def row_block(dy_, dx_):
        return 4 * ((y + dy_) % 2) + 2 * ((x + dx_) % 2) + c

    blocks = [row_block(0, 0), row_block(0, 1), row_block(1, 0), row_block(1, 1)]

    def rcopy(src, dst, ss, rs, dev):
        return pltpu.make_async_remote_copy(
            src_ref=src, dst_ref=dst, send_sem=ss, recv_sem=rs, device_id=(dev,), device_id_type=MESH
        )

    own = pl.ds(0, ROWS)
    far = pl.ds(ROWS, ROWS)
    def stage(i, j, k):
        return (s1g.at[i, j, k] if i < 4 else gcode.at[2 * (i - 4) + k, j]).at[pl.ds(0, 128)]

    def piece(k, i, j):
        src = (x_hbm, dy_hbm)[k].at[pl.ds(128 * i, 128), pl.ds(HALF * j, HALF)]
        return pltpu.make_async_copy(src, stage(i, j, k), in_sem.at[k, i, j])

    ld_si = pltpu.make_async_copy(sinv_hbm.at[z], sinv, lsem)
    for k in range(2):
        for i in range(8):
            for j in range(2):
                piece(k, i, j).start()
    for l in range(3):
        pltpu.make_async_copy(w_hbm.at[l], wbuf.at[l], wsem.at[l]).start()
    ld_si.start()

    barrier = pltpu.get_barrier_semaphore()
    for dev in [z * 8 + (me + k) % 8 for k in range(1, 8)] + z_peer[1:]:
        pl.semaphore_signal(barrier, inc=1, device_id=(dev,), device_id_type=MESH)
    pl.semaphore_wait(barrier, 10)

    def share(n):
        return rcopy(hg.at[n, :, own], hg.at[n, :, far], d2d_s.at[n], d2d_r.at[n], mate)

    def forward(l):
        pltpu.make_async_copy(w_hbm.at[l], wbuf.at[l], wsem.at[l]).wait()

        @pl.loop(0, 3)
        def _(i):
            rows = pl.ds(pl.multiple_of(i * 256, 256), 256)
            pre = lax.dot_general(wbuf[l, :, rows], hg[l, :, own], TN, preferred_element_type=F32).astype(BF16)
            hg[4 + l, rows, own] = pre
            v = pre.astype(F32)
            hg[l + 1, rows, own] = (v * (0.5 * (1.0 + gelu_tanh(v)))).astype(BF16)

        share(l + 1).start()

        @pl.when(l == 0)
        def _():
            pltpu.make_async_copy(w_hbm.at[3], wbuf.at[0], wsem.at[0]).start()

    def backward(l):
        k = l % 3

        @pl.when(l == 3)
        def _():
            pltpu.make_async_copy(w_hbm.at[3], wbuf.at[0], wsem.at[0]).wait()

        @pl.loop(0, 3)
        def _(i):
            rows = pl.ds(pl.multiple_of(i * 256, 256), 256)
            dh = jnp.dot(wbuf[k, rows, :], hg[4 + l, :, own], preferred_element_type=F32).astype(BF16).astype(F32)
            v = hg[3 + l, rows, own].astype(F32)
            t = gelu_tanh(v)
            slope = 0.5 * (1.0 + t) + (0.5 * v) * (1.0 - t * t) * (GELU_C * (1.0 + (3.0 * 0.044715) * (v * v)))
            hg[3 + l, rows, own] = (dh * slope).astype(BF16)

        share(3 + l).start()

    class Red:
        def __init__(self, first, width, acc, accx, s1, r1, r2, zr):
            self.first, self.width = first, width
            self.acc, self.accx, self.s1, self.r1, self.r2, self.zr = acc, accx, s1, r1, r2, zr

        def cols(self, j):
            return pl.ds(j * self.width, self.width)

        def st1(self, m, j):
            k = m - self.first
            return rcopy(self.s1.at[k, j], self.r1.at[k, j], s1_s.at[m, j], s1_r.at[m, j], (x_nbr, y_nbr)[j])

        def st2(self, m, j):
            k = m - self.first
            return rcopy(self.s1.at[k, 0, j], self.r2.at[k, j], s2_s.at[m, j], s2_r.at[m, j], (y_nbr, x_nbr)[j])

        def turn(self, m):
            k = m - self.first
            self.st1(m, 0).wait_send()
            for j in range(2):
                self.st1(m, j).wait_recv()
                put(self.s1, (k, 0, j), self.accx[k, j] + get(self.r1, (k, j, 1)))
                self.st2(m, j).start()
                self.acc[k, :, self.cols(j)] += get(self.r1, (k, j, 0))

        def z_copy(self, m):
            k = m - self.first
            kind = k // 4
            l = m % 4
            slot = (l - z + 3) % 4
            return rcopy(
                self.s1.at[k, 1], self.zr.at[kind, slot], z_s.at[m], z_r.at[m // 4, slot], (me + 8 * (l - z) + 32) % 32
            )

        def across(self, m):
            k = m - self.first
            self.st1(m, 1).wait_send()
            for j in range(2):
                self.st2(m, j).wait_recv()
                total = self.acc[k, :, self.cols(j)] + get(self.r2, (k, j))
                self.acc[k, :, self.cols(j)] = total

                @pl.when(m % 4 != z)
                def _():
                    put(self.s1, (k, 1, j), total)

            @pl.when(m % 4 != z)
            def _():
                self.z_copy(m).start()

        def z_wait(self, kind):
            for k in range(3):
                rcopy(
                    self.s1.at[0, 1], self.zr.at[kind, k], z_s.at[0], z_r.at[kind + self.first // 4, k], z_peer[k + 1]
                ).wait_recv()

        def z_total(self, kind, j):
            t = self.acc[kind * 4 + z, :, self.cols(j)]
            for k in range(3):
                t = t + get(self.zr, (kind, k, j))
            return t

    rg = Red(0, HALF, accg, accxg, s1g, r1g, r2g, zrg)
    rs = Red(4, BHALF, accs, accxs, s1s, r1s, r2s, zrs)

    def product(m):
        kind = m // 4
        l = m % 4
        left = jnp.where(kind == 2, 4 + l, l)
        right = jnp.where(kind == 1, l, 4 + l)
        for d in range(4):
            lhs[pl.ds(OWN * d, OWN), :] = hg[left, pl.ds(pl.multiple_of(blocks[d] * OWN, OWN), OWN), :]

        @pl.loop(0, 2)
        def _(j):
            cols = pl.ds(pl.multiple_of(j * HALF, HALF), HALF)
            full[:, cols] = lax.dot_general(lhs[...], hg[right, cols, :], NT, preferred_element_type=F32)

        def send(red, pieces):
            k = m - red.first
            for j in range(2):
                cols = slice(j * red.width, (j + 1) * red.width)
                near, other = (1, 2) if j == 0 else (2, 1)
                red.acc[k, :, cols] = pieces[0][:, cols]
                put(red.s1, (k, j, 0), pieces[near][:, cols])
                put(red.s1, (k, j, 1), pieces[3][:, cols])
                red.accx[k, j] = pieces[other][:, cols]
                red.st1(m, j).start()

        @pl.when(kind == 0)
        def _():
            send(rg, [full[pl.ds(OWN * d, OWN), :] for d in range(4)])

        @pl.when(kind > 0)
        def _():
            send(rs, [
                pltpu.roll(full[pl.ds(OWN * d, OWN), :], (D - OWN * blocks[d]) % D, 1)[:, :BAND] for d in range(4)
            ])

    def by_kind(name):
        def act(m):
            @pl.when(m < 4)
            def _():
                getattr(rg, name)(m)

            @pl.when(m >= 4)
            def _():
                getattr(rs, name)(m)

        return act

    inv_batch = 1.0 / BATCH

    def gather_copies(ref, base, ss, rs, own_src):
        def at(rb, half=None):
            return ref.at[base + rb] if half is None else ref.at[base + rb, half]

        first = [
            rcopy(own_src, at(blocks[0]), ss.at[0], rs.at[0], x_nbr),
            rcopy(own_src, at(blocks[0]), ss.at[1], rs.at[1], y_nbr),
            rcopy(own_src, at(blocks[0]), ss.at[2], rs.at[2], mate),
        ]
        from_x = [
            rcopy(at(blocks[1], 0), at(blocks[1], 0), ss.at[3], rs.at[3], y_nbr),
            rcopy(at(blocks[1]), at(blocks[1]), ss.at[5], rs.at[5], mate),
        ]
        from_y = [
            rcopy(at(blocks[2], 1), at(blocks[2], 1), ss.at[4], rs.at[4], x_nbr),
            rcopy(at(blocks[2]), at(blocks[2]), ss.at[6], rs.at[6], mate),
        ]
        last = rcopy(at(blocks[3]), at(blocks[3]), ss.at[7], rs.at[7], mate)
        return first, from_x, from_y, last

    def gather_rest(copies):
        first, from_x, from_y, last = copies
        first[0].wait_recv()
        for cp in from_x:
            cp.start()
        first[1].wait_recv()
        for cp in from_y:
            cp.start()

    def gather_last(copies):
        first, from_x, from_y, last = copies
        from_x[0].wait_recv()
        from_y[0].wait_recv()
        last.start()

    def gather_end(copies):
        first, from_x, from_y, last = copies
        for cp in (first[2], from_x[1], from_y[1], last):
            cp.wait_recv()

    def gather_sent(copies):
        first, from_x, from_y, last = copies
        for cp in (*first, *from_x, *from_y, last):
            cp.wait_send()

    g_copies = gather_copies(gcode, 0, g_s, g_r, gcode.at[blocks[0]])

    def u_row(l):
        return u_out.at[l * 8 + blocks[0]]

    def u_copies(k):
        l = (z - k + 4) % 4
        return gather_copies(u_out, l * 8, u_s.at[k], u_r.at[k], u_row(l))

    own_first = gather_copies(u_out, z * 8, u_s.at[0], u_r.at[0], ubuf)[0]
    local = pltpu.make_async_copy(ubuf, u_row(z), us_loc)

    def z_send(k, l):
        return rcopy(ubuf, u_row(l), uz_s.at[k - 1], uz_r.at[k - 1], (me + 8 * k) % 32)

    def own_grad(_):
        rg.z_wait(0)
        for j in range(2):
            put(gcode, (blocks[0], j), rg.z_total(0, j) * inv_batch)
        for cp in g_copies[0]:
            cp.start()

    def precondition(_):
        gather_end(g_copies)

        @pl.loop(0, 8)
        def _(b):
            for j in range(2):
                gfull[pl.ds(pl.multiple_of(b * OWN, OWN), OWN), pl.ds(j * HALF, HALF)] = get(gcode, (b, j))

        ld_si.wait()
        left_prod = jnp.dot(a_inv[...], gfull[...], precision=HIGH, preferred_element_type=F32)
        u_rows = jnp.dot(left_prod, sinv[...], precision=HIGH, preferred_element_type=F32)
        for j in range(2):
            put(ubuf, (j,), u_rows[:, j * HALF : (j + 1) * HALF])
        for k in range(1, 4):
            z_send(k, z).start()
        for cp in own_first:
            cp.start()
        local.start()

    def from_plane(k):
        z_send(k, (z - k + 4) % 4).wait_recv()
        for cp in u_copies(k)[0]:
            cp.start()

    def flip_copy(kind, e):
        return rcopy(
            flip.at[kind, e - 1], f_flip.at[kind, e - 1], t_s.at[kind, e - 1], t_r.at[kind, e - 1],
            z * 8 + (blocks[0] + e) % 8,
        )

    def factors(_):
        for kind in range(2):
            rs.z_wait(kind)
            for j in range(2):
                f_sum[kind, :, rs.cols(j)] = rs.z_total(kind, j)
            turned = f_sum[kind].T
            for e in range(1, 4):
                flip[kind, e - 1, :, pl.ds(0, OWN)] = turned[OWN * e : OWN * (e + 1)]
                flip_copy(kind, e).start()

    def factors_end():
        for kind in range(2):
            for e in range(1, 4):
                flip_copy(kind, e).wait()

    def turn_rows(k, n):
        for i in range(8):
            for j in range(2):
                piece(k, i, j).wait()
                hg[n, pl.ds(j * HALF, HALF), pl.ds(i * 128, 128)] = stage(i, j, k)[...].T

        share(n).start()

    turn_rows(0, 0)

    actions = {
        F: forward,
        B: backward,
        W: lambda n: share(n).wait_recv(),
        PR: product,
        T: by_kind("turn"),
        C: by_kind("across"),
        Z: own_grad,
        R: lambda _: gather_rest(g_copies),
        U: precondition,
        Y: from_plane,
        V: lambda k: gather_rest(u_copies(k)),
        AS: factors,
        RQ: lambda _: gather_last(g_copies),
        VQ: lambda k: gather_last(u_copies(k)),
        DY: lambda _: turn_rows(1, 7),
    }

    @pl.loop(0, len(EVENTS))
    def _(step):
        third, which = step // 3, step % 3
        word = jnp.int32(0)
        for w, packed in enumerate(PLAN):
            word = jnp.where(third == w, packed, word)
        code = jnp.where(which == 0, word % 256, jnp.where(which == 1, (word // 256) % 256, word // 65536))
        op = code // 16
        arg = code % 16
        for o, act in actions.items():

            @pl.when(op == o)
            def _(act=act):
                act(arg)

    @pl.loop(0, 4)
    def _(k):
        gather_end(u_copies(k))
        gather_sent(u_copies(k))

    for k in range(1, 4):
        z_send(k, z).wait_send()
    local.wait()
    gather_sent(g_copies)

    @pl.loop(0, 8)
    def _(n):
        share(n).wait_send()

    factors_end()

    @pl.loop(0, 12)
    def _(m):
        def sent(red):
            for j in range(2):
                red.st2(m, j).wait_send()

            @pl.when(m % 4 != z)
            def _():
                red.z_copy(m).wait_send()

        @pl.when(m < 4)
        def _():
            sent(rg)

        @pl.when(m >= 4)
        def _():
            sent(rs)


PARTS = 8
PER = LAYERS * 8 // PARTS


def finish(code_hbm, a_old, s_old, f_sum, f_flip, rows_hbm, a_new, s_new, code, rows, old, tot, flip, in_sem, out_sem, f_sem):
    def load(i):
        return pltpu.make_async_copy(code_hbm.at[pl.ds(i * PER, PER)], code.at[pl.ds(i * PER, PER)], in_sem.at[i])

    def store(i):
        part = pl.ds(pl.multiple_of(i * PER * OWN, OWN), PER * OWN)
        return pltpu.make_async_copy(rows.at[part], rows_hbm.at[part], out_sem.at[i])

    pairs = ((a_old, a_new), (s_old, s_new))
    moves = [pltpu.make_async_copy(o, old.at[k], f_sem.at[k]) for k, (o, _) in enumerate(pairs)]
    moves.append(pltpu.make_async_copy(f_sum, tot.at[:, :, pl.ds(0, BAND)], f_sem.at[2]))
    moves.append(pltpu.make_async_copy(f_flip, flip, f_sem.at[3]))
    outs = [pltpu.make_async_copy(old.at[k], n, f_sem.at[4 + k]) for k, (_, n) in enumerate(pairs)]
    for cp in moves:
        cp.start()
    for i in range(PARTS):
        load(i).start()
    for cp in moves:
        cp.wait()
    shift = OWN * (lax.axis_index("data") % 8)
    for k in range(2):
        for e in range(1, 4):
            at = D - OWN * e
            tot[k, :, at : at + OWN] = flip[k, e - 1, :, 0:OWN]
        old[k] = DECAY * old[k] + ((1.0 - DECAY) / BATCH) * pltpu.roll(tot[k], shift, 1)
        outs[k].start()

    @pl.loop(0, PARTS)
    def _(i):
        load(i).wait()
        for b in range(PER):
            n = i * PER + b
            for j in range(2):
                rows[pl.ds(pl.multiple_of(n * OWN, OWN), OWN), pl.ds(j * HALF, HALF)] = get(code, (n, j))
        store(i).start()

    for cp in outs:
        cp.wait()
    for i in range(PARTS):
        store(i).wait()


def solution(mesh):
    def device_step(x_loc, dy_loc, weights, a_old_rows, s_old_rows, a_inv_rows, s_inv):
        hbm = pl.BlockSpec(memory_space=pltpu.HBM)
        vmem = pl.BlockSpec(memory_space=pltpu.VMEM)
        dma = pltpu.SemaphoreType.DMA
        u_code, f_sum, f_flip = pl.pallas_call(
            kernel,
            out_shape=(
                jax.ShapeDtypeStruct((LAYERS * 8, 2, CODE, HALF), BF16),
                jax.ShapeDtypeStruct((2, OWN, BAND), F32),
                jax.ShapeDtypeStruct((2, 3, OWN, 128), F32),
            ),
            in_specs=[hbm] * 4 + [vmem],
            out_specs=(hbm, vmem, hbm),
            scratch_shapes=[
                pltpu.VMEM((2 * LAYERS, D, 2 * ROWS), BF16),
                pltpu.VMEM((3, D, D), BF16),
                pltpu.VMEM((4 * OWN, 2 * ROWS), BF16),
                pltpu.VMEM((4 * OWN, D), F32),
                pltpu.VMEM((4, OWN, D), F32),
                pltpu.VMEM((4, 2, OWN, HALF), F32),
                pltpu.VMEM((4, 2, 2, CODE, HALF), BF16),
                pltpu.VMEM((4, 2, 2, CODE, HALF), BF16),
                pltpu.VMEM((4, 2, CODE, HALF), BF16),
                pltpu.VMEM((1, 3, 2, CODE, HALF), BF16),
                pltpu.VMEM((8, OWN, BAND), F32),
                pltpu.VMEM((8, 2, OWN, BHALF), F32),
                pltpu.VMEM((8, 2, 2, SCODE, BHALF), BF16),
                pltpu.VMEM((8, 2, 2, SCODE, BHALF), BF16),
                pltpu.VMEM((8, 2, SCODE, BHALF), BF16),
                pltpu.VMEM((2, 3, 2, SCODE, BHALF), BF16),
                pltpu.VMEM((2, 3, OWN, 128), F32),
                pltpu.VMEM((8, 2, CODE, HALF), BF16),
                pltpu.VMEM((D, D), F32),
                pltpu.VMEM((D, D), F32),
                pltpu.VMEM((2, CODE, HALF), BF16),
                dma((2, 8, 2)),
                dma,
                dma((3,)),
                dma((8,)), dma((8,)),
                dma((12, 2)), dma((12, 2)),
                dma((12, 2)), dma((12, 2)),
                dma((12,)), dma((3, 3)),
                dma((2, 3)), dma((2, 3)),
                dma((8,)), dma((8,)),
                dma((3,)), dma((3,)),
                dma((4, 8)), dma((4, 8)),
                dma,
            ],
            compiler_params=pltpu.CompilerParams(
                collective_id=0, has_side_effects=True, vmem_limit_bytes=67_000_000
            ),
        )(x_loc, dy_loc, weights, s_inv, a_inv_rows)
        own_shape = jax.ShapeDtypeStruct((OWN, D), F32)
        u_rows, a_new, s_new = pl.pallas_call(
            finish,
            out_shape=(jax.ShapeDtypeStruct((LAYERS * D, D), F32), own_shape, own_shape),
            in_specs=[hbm] * 5,
            out_specs=(hbm, hbm, hbm),
            scratch_shapes=[
                pltpu.VMEM((LAYERS * 8, 2, CODE, HALF), BF16),
                pltpu.VMEM((LAYERS * D, D), F32),
                pltpu.VMEM((2, OWN, D), F32),
                pltpu.VMEM((2, OWN, D), F32),
                pltpu.VMEM((2, 3, OWN, 128), F32),
                dma((PARTS,)),
                dma((PARTS,)),
                dma((6,)),
            ],
            compiler_params=pltpu.CompilerParams(vmem_limit_bytes=67_000_000),
        )(u_code, a_old_rows, s_old_rows, f_sum, f_flip)
        return u_rows.reshape(LAYERS, D, D), a_new, s_new

    row_spec = P("data", None)
    return jax.shard_map(
        device_step,
        mesh=mesh,
        in_specs=(row_spec, row_spec, P(), row_spec, row_spec, row_spec, P()),
        out_specs=(P(), row_spec, row_spec),
        check_vma=False,
    )
```

```python
import math
import jax
import jax.numpy as jnp
from jax import lax
from jax.experimental import pallas as pl
from jax.experimental.pallas import tpu as pltpu
from jax.sharding import PartitionSpec as P

DECAY = 0.75
F32 = jnp.float32
BF16 = jnp.bfloat16
MESH = pl.DeviceIdType.MESH
HIGH = lax.Precision.HIGHEST
LAYERS = 4
D = 768
ROWS = 1024
BATCH = 32 * ROWS
OWN = 96
HALF = 384
BAND = 512
BHALF = BAND // 2
GELU_C = math.sqrt(2.0 / math.pi)
NT = (((1,), (1,)), ((), ()))
TN = (((0,), (0,)), ((), ()))

STEPS = {2: 2560.0, 3: 768.0}
BASE = {2: 21.0, 3: 7.0}
CODE = OWN + OWN // 2
SCODE = OWN + OWN // 3


def nearest(v):
    return (v + 12582912.0) - 12582912.0


def encode(v, group):
    hi = v.astype(BF16)
    h = hi.astype(F32)
    bound = STEPS[group] / 256.0
    q = nearest(jnp.clip((v - h) / jnp.where(h == 0.0, 1.0, h) * STEPS[group], -bound, bound))
    n = OWN // group
    word = q[:n]
    for k in range(1, group):
        word = word * BASE[group] + q[k * n : (k + 1) * n]
    return hi, word.astype(BF16)


def decode(hi, lo, group):
    h = hi.astype(F32)
    w = lo.astype(F32)
    parts = []
    for k in range(group - 1, 0, -1):
        unit = BASE[group] ** k
        parts.append(nearest(w * (1.0 / unit)))
        w = w - unit * parts[-1]
    q = jnp.concatenate([*parts, w], axis=-2)
    return h + h * (q * (1.0 / STEPS[group]))


def rows_of(ref):
    return ref.shape[-2], OWN // (ref.shape[-2] - OWN)


def put(ref, idx, v):
    rows, group = rows_of(ref)
    hi, lo = encode(v, group)
    ref[(*idx, slice(0, OWN))] = hi
    ref[(*idx, slice(OWN, rows))] = lo


def get(ref, idx):
    rows, group = rows_of(ref)
    return decode(ref[(*idx, slice(0, OWN))], ref[(*idx, slice(OWN, rows))], group)


def gelu_tanh(v):
    return jnp.tanh(GELU_C * (v + 0.044715 * (v * v * v)))


F, B, W, PR, T, C, Z, R, U, Y, V, AS, RQ, VQ, DY = range(15)
EVENTS = [
    (F, 0), (DY, 0), (F, 1), (F, 2), (W, 7), (PR, 11), (B, 3), (W, 3), (PR, 3), (B, 2),
    (W, 2), (W, 6), (PR, 2), (B, 1), (W, 1), (W, 5), (PR, 1), (W, 0), (W, 4), (PR, 0),
    (T, 1), (T, 3), (PR, 5), (T, 0), (C, 1), (T, 2), (PR, 10), (C, 3), (PR, 6), (C, 0),
    (PR, 7), (PR, 9), (T, 5), (T, 11), (C, 2), (Z, 0), (R, 0), (C, 5), (PR, 8), (T, 7),
    (RQ, 0), (C, 11), (T, 9), (T, 6), (U, 0), (PR, 4), (T, 8), (V, 0), (T, 4), (C, 6),
    (T, 10), (Y, 1), (C, 9), (Y, 2), (C, 4), (V, 1), (C, 8), (Y, 3), (C, 10), (V, 2),
    (C, 7), (VQ, 0), (V, 3), (VQ, 1), (VQ, 2), (AS, 0), (VQ, 3),
]
CODES = [op * 16 + arg for op, arg in EVENTS]
CODES += [0] * (-len(CODES) % 3)
PLAN = [a + 256 * b + 65536 * c for a, b, c in zip(CODES[::3], CODES[1::3], CODES[2::3])]


def kernel(
    x_hbm, dy_hbm, w_hbm, sinv_hbm, a_inv,
    u_out, f_sum, f_flip,
    hg, wbuf, lhs, full, accg, accxg, s1g, r1g, r2g, zrg, accs, accxs, s1s, r1s, r2s, zrs, flip, gcode, gfull, sinv, ubuf,
    in_sem, lsem, wsem, d2d_s, d2d_r, s1_s, s1_r, s2_s, s2_r, z_s, z_r, t_s, t_r, g_s, g_r, uz_s, uz_r, u_s, u_r, us_loc,
):
    me = lax.axis_index("data")
    c = me % 2
    x = (me // 2) % 2
    y = (me // 4) % 2
    z = me // 8
    mate = me + 1 - 2 * c
    x_nbr = me + 2 - 4 * x
    y_nbr = me + 4 - 8 * y
    z_peer = [(me + 8 * k) % 32 for k in range(4)]

    def row_block(dy_, dx_):
        return 4 * ((y + dy_) % 2) + 2 * ((x + dx_) % 2) + c

    blocks = [row_block(0, 0), row_block(0, 1), row_block(1, 0), row_block(1, 1)]

    def rcopy(src, dst, ss, rs, dev):
        return pltpu.make_async_remote_copy(
            src_ref=src, dst_ref=dst, send_sem=ss, recv_sem=rs, device_id=(dev,), device_id_type=MESH
        )

    own = pl.ds(0, ROWS)
    far = pl.ds(ROWS, ROWS)
    def stage(i, j, k):
        return (s1g.at[i, j, k] if i < 4 else gcode.at[2 * (i - 4) + k, j]).at[pl.ds(0, 128)]

    def piece(k, i, j):
        src = (x_hbm, dy_hbm)[k].at[pl.ds(128 * i, 128), pl.ds(HALF * j, HALF)]
        return pltpu.make_async_copy(src, stage(i, j, k), in_sem.at[k, i, j])

    ld_si = pltpu.make_async_copy(sinv_hbm.at[z], sinv, lsem)
    for k in range(2):
        for i in range(8):
            for j in range(2):
                piece(k, i, j).start()
    for l in range(3):
        pltpu.make_async_copy(w_hbm.at[l], wbuf.at[l], wsem.at[l]).start()
    ld_si.start()

    barrier = pltpu.get_barrier_semaphore()
    for dev in [z * 8 + (me + k) % 8 for k in range(1, 8)] + z_peer[1:]:
        pl.semaphore_signal(barrier, inc=1, device_id=(dev,), device_id_type=MESH)
    pl.semaphore_wait(barrier, 10)

    def share(n):
        return rcopy(hg.at[n, :, own], hg.at[n, :, far], d2d_s.at[n], d2d_r.at[n], mate)

    def forward(l):
        pltpu.make_async_copy(w_hbm.at[l], wbuf.at[l], wsem.at[l]).wait()

        pre = lax.dot_general(wbuf[l], hg[l, :, own], TN, preferred_element_type=F32).astype(BF16)
        hg[4 + l, :, own] = pre
        v = pre.astype(F32)
        hg[l + 1, :, own] = (v * (0.5 * (1.0 + gelu_tanh(v)))).astype(BF16)

        share(l + 1).start()

        @pl.when(l == 0)
        def _():
            pltpu.make_async_copy(w_hbm.at[3], wbuf.at[0], wsem.at[0]).start()

    def backward(l):
        k = l % 3

        @pl.when(l == 3)
        def _():
            pltpu.make_async_copy(w_hbm.at[3], wbuf.at[0], wsem.at[0]).wait()

        @pl.loop(0, 2)
        def _(i):
            rows = pl.ds(pl.multiple_of(i * 384, 384), 384)
            dh = jnp.dot(wbuf[k, rows, :], hg[4 + l, :, own], preferred_element_type=F32).astype(BF16).astype(F32)
            v = hg[3 + l, rows, own].astype(F32)
            t = gelu_tanh(v)
            slope = 0.5 * (1.0 + t) + (0.5 * v) * (1.0 - t * t) * (GELU_C * (1.0 + (3.0 * 0.044715) * (v * v)))
            hg[3 + l, rows, own] = (dh * slope).astype(BF16)

        share(3 + l).start()

    class Red:
        def __init__(self, first, width, acc, accx, s1, r1, r2, zr):
            self.first, self.width = first, width
            self.acc, self.accx, self.s1, self.r1, self.r2, self.zr = acc, accx, s1, r1, r2, zr

        def cols(self, j):
            return pl.ds(j * self.width, self.width)

        def st1(self, m, j):
            k = m - self.first
            return rcopy(self.s1.at[k, j], self.r1.at[k, j], s1_s.at[m, j], s1_r.at[m, j], (x_nbr, y_nbr)[j])

        def st2(self, m, j):
            k = m - self.first
            return rcopy(self.s1.at[k, 0, j], self.r2.at[k, j], s2_s.at[m, j], s2_r.at[m, j], (y_nbr, x_nbr)[j])

        def turn(self, m):
            k = m - self.first
            self.st1(m, 0).wait_send()
            for j in range(2):
                self.st1(m, j).wait_recv()
                put(self.s1, (k, 0, j), self.accx[k, j] + get(self.r1, (k, j, 1)))
                self.st2(m, j).start()
                self.acc[k, :, self.cols(j)] += get(self.r1, (k, j, 0))

        def z_copy(self, m):
            k = m - self.first
            kind = k // 4
            l = m % 4
            slot = (l - z + 3) % 4
            return rcopy(
                self.s1.at[k, 1], self.zr.at[kind, slot], z_s.at[m], z_r.at[m // 4, slot], (me + 8 * (l - z) + 32) % 32
            )

        def across(self, m):
            k = m - self.first
            self.st1(m, 1).wait_send()
            for j in range(2):
                self.st2(m, j).wait_recv()
                total = self.acc[k, :, self.cols(j)] + get(self.r2, (k, j))
                self.acc[k, :, self.cols(j)] = total

                @pl.when(m % 4 != z)
                def _():
                    put(self.s1, (k, 1, j), total)

            @pl.when(m % 4 != z)
            def _():
                self.z_copy(m).start()

        def z_wait(self, kind):
            for k in range(3):
                rcopy(
                    self.s1.at[0, 1], self.zr.at[kind, k], z_s.at[0], z_r.at[kind + self.first // 4, k], z_peer[k + 1]
                ).wait_recv()

        def z_total(self, kind, j):
            t = self.acc[kind * 4 + z, :, self.cols(j)]
            for k in range(3):
                t = t + get(self.zr, (kind, k, j))
            return t

    rg = Red(0, HALF, accg, accxg, s1g, r1g, r2g, zrg)
    rs = Red(4, BHALF, accs, accxs, s1s, r1s, r2s, zrs)

    def product(m):
        kind = m // 4
        l = m % 4
        left = jnp.where(kind == 2, 4 + l, l)
        right = jnp.where(kind == 1, l, 4 + l)
        for d in range(4):
            lhs[pl.ds(OWN * d, OWN), :] = hg[left, pl.ds(pl.multiple_of(blocks[d] * OWN, OWN), OWN), :]

        full[...] = lax.dot_general(lhs[...], hg[right], NT, preferred_element_type=F32)

        def send(red, pieces):
            k = m - red.first
            for j in range(2):
                cols = slice(j * red.width, (j + 1) * red.width)
                near, other = (1, 2) if j == 0 else (2, 1)
                red.acc[k, :, cols] = pieces[0][:, cols]
                put(red.s1, (k, j, 0), pieces[near][:, cols])
                put(red.s1, (k, j, 1), pieces[3][:, cols])
                red.accx[k, j] = pieces[other][:, cols]
                red.st1(m, j).start()

        @pl.when(kind == 0)
        def _():
            send(rg, [full[pl.ds(OWN * d, OWN), :] for d in range(4)])

        @pl.when(kind > 0)
        def _():
            send(rs, [
                pltpu.roll(full[pl.ds(OWN * d, OWN), :], (D - OWN * blocks[d]) % D, 1)[:, :BAND] for d in range(4)
            ])

    def by_kind(name):
        def act(m):
            @pl.when(m < 4)
            def _():
                getattr(rg, name)(m)

            @pl.when(m >= 4)
            def _():
                getattr(rs, name)(m)

        return act

    inv_batch = 1.0 / BATCH

    def gather_copies(ref, base, ss, rs, own_src):
        def at(rb, half=None):
            return ref.at[base + rb] if half is None else ref.at[base + rb, half]

        first = [
            rcopy(own_src, at(blocks[0]), ss.at[0], rs.at[0], x_nbr),
            rcopy(own_src, at(blocks[0]), ss.at[1], rs.at[1], y_nbr),
            rcopy(own_src, at(blocks[0]), ss.at[2], rs.at[2], mate),
        ]
        from_x = [
            rcopy(at(blocks[1], 0), at(blocks[1], 0), ss.at[3], rs.at[3], y_nbr),
            rcopy(at(blocks[1]), at(blocks[1]), ss.at[5], rs.at[5], mate),
        ]
        from_y = [
            rcopy(at(blocks[2], 1), at(blocks[2], 1), ss.at[4], rs.at[4], x_nbr),
            rcopy(at(blocks[2]), at(blocks[2]), ss.at[6], rs.at[6], mate),
        ]
        last = rcopy(at(blocks[3]), at(blocks[3]), ss.at[7], rs.at[7], mate)
        return first, from_x, from_y, last

    def gather_rest(copies):
        first, from_x, from_y, last = copies
        first[0].wait_recv()
        for cp in from_x:
            cp.start()
        first[1].wait_recv()
        for cp in from_y:
            cp.start()

    def gather_last(copies):
        first, from_x, from_y, last = copies
        from_x[0].wait_recv()
        from_y[0].wait_recv()
        last.start()

    def gather_end(copies):
        first, from_x, from_y, last = copies
        for cp in (first[2], from_x[1], from_y[1], last):
            cp.wait_recv()

    def gather_sent(copies):
        first, from_x, from_y, last = copies
        for cp in (*first, *from_x, *from_y, last):
            cp.wait_send()

    g_copies = gather_copies(gcode, 0, g_s, g_r, gcode.at[blocks[0]])

    def u_row(l):
        return u_out.at[l * 8 + blocks[0]]

    def u_copies(k):
        l = (z - k + 4) % 4
        return gather_copies(u_out, l * 8, u_s.at[k], u_r.at[k], u_row(l))

    own_first = gather_copies(u_out, z * 8, u_s.at[0], u_r.at[0], ubuf)[0]
    local = pltpu.make_async_copy(ubuf, u_row(z), us_loc)

    def z_send(k, l):
        return rcopy(ubuf, u_row(l), uz_s.at[k - 1], uz_r.at[k - 1], (me + 8 * k) % 32)

    def own_grad(_):
        rg.z_wait(0)
        for j in range(2):
            put(gcode, (blocks[0], j), rg.z_total(0, j) * inv_batch)
        for cp in g_copies[0]:
            cp.start()

    def precondition(_):
        gather_end(g_copies)

        @pl.loop(0, 8)
        def _(b):
            for j in range(2):
                gfull[pl.ds(pl.multiple_of(b * OWN, OWN), OWN), pl.ds(j * HALF, HALF)] = get(gcode, (b, j))

        ld_si.wait()
        left_prod = jnp.dot(a_inv[...], gfull[...], precision=HIGH, preferred_element_type=F32)
        u_rows = jnp.dot(left_prod, sinv[...], precision=HIGH, preferred_element_type=F32)
        for j in range(2):
            put(ubuf, (j,), u_rows[:, j * HALF : (j + 1) * HALF])
        for k in range(1, 4):
            z_send(k, z).start()
        for cp in own_first:
            cp.start()
        local.start()

    def from_plane(k):
        z_send(k, (z - k + 4) % 4).wait_recv()
        for cp in u_copies(k)[0]:
            cp.start()

    def flip_copy(kind, e):
        return rcopy(
            flip.at[kind, e - 1], f_flip.at[kind, e - 1], t_s.at[kind, e - 1], t_r.at[kind, e - 1],
            z * 8 + (blocks[0] + e) % 8,
        )

    def factors(_):
        for kind in range(2):
            rs.z_wait(kind)
            for j in range(2):
                f_sum[kind, :, rs.cols(j)] = rs.z_total(kind, j)
            turned = f_sum[kind].T
            for e in range(1, 4):
                flip[kind, e - 1, :, pl.ds(0, OWN)] = turned[OWN * e : OWN * (e + 1)]
                flip_copy(kind, e).start()

    def factors_end():
        for kind in range(2):
            for e in range(1, 4):
                flip_copy(kind, e).wait()

    def turn_rows(k, n):
        for i in range(8):
            for j in range(2):
                piece(k, i, j).wait()
                hg[n, pl.ds(j * HALF, HALF), pl.ds(i * 128, 128)] = stage(i, j, k)[...].T

        share(n).start()

    turn_rows(0, 0)

    actions = {
        F: forward,
        B: backward,
        W: lambda n: share(n).wait_recv(),
        PR: product,
        T: by_kind("turn"),
        C: by_kind("across"),
        Z: own_grad,
        R: lambda _: gather_rest(g_copies),
        U: precondition,
        Y: from_plane,
        V: lambda k: gather_rest(u_copies(k)),
        AS: factors,
        RQ: lambda _: gather_last(g_copies),
        VQ: lambda k: gather_last(u_copies(k)),
        DY: lambda _: turn_rows(1, 7),
    }

    @pl.loop(0, len(EVENTS))
    def _(step):
        third, which = step // 3, step % 3
        word = jnp.int32(0)
        for w, packed in enumerate(PLAN):
            word = jnp.where(third == w, packed, word)
        code = jnp.where(which == 0, word % 256, jnp.where(which == 1, (word // 256) % 256, word // 65536))
        op = code // 16
        arg = code % 16
        for o, act in actions.items():

            @pl.when(op == o)
            def _(act=act):
                act(arg)

    @pl.loop(0, 4)
    def _(k):
        gather_end(u_copies(k))
        gather_sent(u_copies(k))

    for k in range(1, 4):
        z_send(k, z).wait_send()
    local.wait()
    gather_sent(g_copies)

    @pl.loop(0, 8)
    def _(n):
        share(n).wait_send()

    factors_end()

    @pl.loop(0, 12)
    def _(m):
        def sent(red):
            for j in range(2):
                red.st2(m, j).wait_send()

            @pl.when(m % 4 != z)
            def _():
                red.z_copy(m).wait_send()

        @pl.when(m < 4)
        def _():
            sent(rg)

        @pl.when(m >= 4)
        def _():
            sent(rs)


PARTS = 8
PER = LAYERS * 8 // PARTS


def finish(code_hbm, a_old, s_old, f_sum, f_flip, rows_hbm, a_new, s_new, code, rows, old, tot, flip, in_sem, out_sem, f_sem):
    def load(i):
        return pltpu.make_async_copy(code_hbm.at[pl.ds(i * PER, PER)], code.at[pl.ds(i * PER, PER)], in_sem.at[i])

    def store(i):
        part = pl.ds(pl.multiple_of(i * PER * OWN, OWN), PER * OWN)
        return pltpu.make_async_copy(rows.at[part], rows_hbm.at[part], out_sem.at[i])

    pairs = ((a_old, a_new), (s_old, s_new))
    moves = [pltpu.make_async_copy(o, old.at[k], f_sem.at[k]) for k, (o, _) in enumerate(pairs)]
    moves.append(pltpu.make_async_copy(f_sum, tot.at[:, :, pl.ds(0, BAND)], f_sem.at[2]))
    moves.append(pltpu.make_async_copy(f_flip, flip, f_sem.at[3]))
    outs = [pltpu.make_async_copy(old.at[k], n, f_sem.at[4 + k]) for k, (_, n) in enumerate(pairs)]
    for cp in moves:
        cp.start()
    for i in range(PARTS):
        load(i).start()
    for cp in moves:
        cp.wait()
    shift = OWN * (lax.axis_index("data") % 8)
    for k in range(2):
        for e in range(1, 4):
            at = D - OWN * e
            tot[k, :, at : at + OWN] = flip[k, e - 1, :, 0:OWN]
        old[k] = DECAY * old[k] + ((1.0 - DECAY) / BATCH) * pltpu.roll(tot[k], shift, 1)
        outs[k].start()

    @pl.loop(0, PARTS)
    def _(i):
        load(i).wait()
        for b in range(PER):
            n = i * PER + b
            for j in range(2):
                rows[pl.ds(pl.multiple_of(n * OWN, OWN), OWN), pl.ds(j * HALF, HALF)] = get(code, (n, j))
        store(i).start()

    for cp in outs:
        cp.wait()
    for i in range(PARTS):
        store(i).wait()


def solution(mesh):
    def device_step(x_loc, dy_loc, weights, a_old_rows, s_old_rows, a_inv_rows, s_inv):
        hbm = pl.BlockSpec(memory_space=pltpu.HBM)
        vmem = pl.BlockSpec(memory_space=pltpu.VMEM)
        dma = pltpu.SemaphoreType.DMA
        u_code, f_sum, f_flip = pl.pallas_call(
            kernel,
            out_shape=(
                jax.ShapeDtypeStruct((LAYERS * 8, 2, CODE, HALF), BF16),
                jax.ShapeDtypeStruct((2, OWN, BAND), F32),
                jax.ShapeDtypeStruct((2, 3, OWN, 128), F32),
            ),
            in_specs=[hbm] * 4 + [vmem],
            out_specs=(hbm, vmem, hbm),
            scratch_shapes=[
                pltpu.VMEM((2 * LAYERS, D, 2 * ROWS), BF16),
                pltpu.VMEM((3, D, D), BF16),
                pltpu.VMEM((4 * OWN, 2 * ROWS), BF16),
                pltpu.VMEM((4 * OWN, D), F32),
                pltpu.VMEM((4, OWN, D), F32),
                pltpu.VMEM((4, 2, OWN, HALF), F32),
                pltpu.VMEM((4, 2, 2, CODE, HALF), BF16),
                pltpu.VMEM((4, 2, 2, CODE, HALF), BF16),
                pltpu.VMEM((4, 2, CODE, HALF), BF16),
                pltpu.VMEM((1, 3, 2, CODE, HALF), BF16),
                pltpu.VMEM((8, OWN, BAND), F32),
                pltpu.VMEM((8, 2, OWN, BHALF), F32),
                pltpu.VMEM((8, 2, 2, SCODE, BHALF), BF16),
                pltpu.VMEM((8, 2, 2, SCODE, BHALF), BF16),
                pltpu.VMEM((8, 2, SCODE, BHALF), BF16),
                pltpu.VMEM((2, 3, 2, SCODE, BHALF), BF16),
                pltpu.VMEM((2, 3, OWN, 128), F32),
                pltpu.VMEM((8, 2, CODE, HALF), BF16),
                pltpu.VMEM((D, D), F32),
                pltpu.VMEM((D, D), F32),
                pltpu.VMEM((2, CODE, HALF), BF16),
                dma((2, 8, 2)),
                dma,
                dma((3,)),
                dma((8,)), dma((8,)),
                dma((12, 2)), dma((12, 2)),
                dma((12, 2)), dma((12, 2)),
                dma((12,)), dma((3, 3)),
                dma((2, 3)), dma((2, 3)),
                dma((8,)), dma((8,)),
                dma((3,)), dma((3,)),
                dma((4, 8)), dma((4, 8)),
                dma,
            ],
            compiler_params=pltpu.CompilerParams(
                collective_id=0, has_side_effects=True, vmem_limit_bytes=67_000_000
            ),
        )(x_loc, dy_loc, weights, s_inv, a_inv_rows)
        own_shape = jax.ShapeDtypeStruct((OWN, D), F32)
        u_rows, a_new, s_new = pl.pallas_call(
            finish,
            out_shape=(jax.ShapeDtypeStruct((LAYERS * D, D), F32), own_shape, own_shape),
            in_specs=[hbm] * 5,
            out_specs=(hbm, hbm, hbm),
            scratch_shapes=[
                pltpu.VMEM((LAYERS * 8, 2, CODE, HALF), BF16),
                pltpu.VMEM((LAYERS * D, D), F32),
                pltpu.VMEM((2, OWN, D), F32),
                pltpu.VMEM((2, OWN, D), F32),
                pltpu.VMEM((2, 3, OWN, 128), F32),
                dma((PARTS,)),
                dma((PARTS,)),
                dma((6,)),
            ],
            compiler_params=pltpu.CompilerParams(vmem_limit_bytes=67_000_000),
        )(u_code, a_old_rows, s_old_rows, f_sum, f_flip)
        return u_rows.reshape(LAYERS, D, D), a_new, s_new

    row_spec = P("data", None)
    return jax.shard_map(
        device_step,
        mesh=mesh,
        in_specs=(row_spec, row_spec, P(), row_spec, row_spec, row_spec, P()),
        out_specs=(P(), row_spec, row_spec),
        check_vma=False,
    )
```
